256 devices in a mesh: dp: 8 (over y, core), vocab: 32 (over x, z).
Axes of the slice: x: 4, y: 4, z: 8, core: 2. Of those that a mesh axis runs over, the one named last changes fastest.
Arguments:
- hidden: bfloat16 [512, 3584], P('dp'), may hold values from -48 to 48
- embedding: bfloat16 [196608, 3584], P(('dp', 'vocab')), may hold values from -1 to 1
- targets: int32 [512], P('dp'), may hold values from 0 to 196607
- loss_weight: bfloat16 [512], P('dp'), may hold values from 1 to 10
Outputs:
- hidden_grad: bfloat16 [512, 3584], P('dp')
- table_grad: bfloat16 [196608, 3584], P(('dp', 'vocab'))
The draws below stay inside these ranges and needn't reach their ends.
All inputs are finite; a program needn't handle non-finite values.
Results may differ from the reference program's by a relative error of at most 0.0049.
Values may be sent and summed in bfloat16 or wider, within the bound.
A program may use at most 128 MiB of HBM per device.

```python
import math
import jax
import jax.numpy as jnp
import numpy as np
from jax import lax

D = 3584
VROWS = 768
VOCAB = 196608
TOKENS = 512
N_VOCAB = 32


def draw_hidden(key, part):
    noise = jnp.clip(jax.random.normal(jax.random.fold_in(key, 11), (TOKENS, D), jnp.float32), -6.0, 6.0)
    return noise.astype(jnp.bfloat16)


def draw_embedding(key, part):
    noise = jnp.clip(jax.random.normal(jax.random.fold_in(key, 13), (VOCAB, D), jnp.float32), -6.0, 6.0)
    place = jnp.arange(VOCAB, dtype=jnp.float32) / (VOCAB - 1)
    rising = jnp.sqrt(1.0 + 0.245 * place)
    table = noise * (3.0 / math.sqrt(D))
    return jnp.clip(table * rising[:, None], -1.0, 1.0).astype(jnp.bfloat16)


def plant(drawn, stream_key, low, top_value):
    extent = drawn.shape
    spot = [jax.random.randint(jax.random.fold_in(stream_key, axis), (), 0, extent[axis]) for axis in range(len(extent))]
    drawn = drawn.at[tuple(spot)].set(low)
    longest = extent.index(max(extent))
    spot[longest] = (spot[longest] + 1) % extent[longest]
    return drawn.at[tuple(spot)].set(top_value)


def levels(own_key, dims, pieces, low, top_value):
    gain, own = 1.0, jax.random.fold_in(own_key, 6)
    for position, parts in pieces:
        draws = jnp.exp(jax.random.uniform(jax.random.fold_in(own, position), (parts,), jnp.float32, low / len(pieces), top_value / len(pieces)))
        gain = gain * jnp.repeat(draws, dims[position] // parts).reshape([-1 if axis == position else 1 for axis in range(len(dims))])
    return gain


def skewed_wide(key, extent, number_of, skew):
    loads = [min(1 << octave, number_of + 1 - (1 << octave)) * (1 << 20) // math.isqrt((1 << octave) ** skew) + 1 for octave in range((number_of + 1).bit_length()) if 1 << octave <= number_of]
    scale = 1 + sum(loads) // (1 << 30)
    grid = np.cumsum(np.array([max(1, weight // scale) for weight in loads]))
    pick = jax.random.randint(jax.random.fold_in(key, 1), extent, 0, int(grid[len(loads) - 1]))
    start = jnp.left_shift(1, jnp.searchsorted(jnp.asarray(grid, jnp.int32), pick, side="right").astype(jnp.int32))
    standing = start - 1 + jax.random.randint(jax.random.fold_in(key, 4), extent, 0, 1 << 30) % jnp.minimum(start, number_of + 1 - start)
    return jax.random.permutation(jax.random.fold_in(key, 2), number_of)[standing].astype(jnp.int32)


def setup_inputs(seed: int = 0) -> dict:
    keys = jax.random.split(jax.random.key(seed), 5)
    hidden = draw_hidden(jax.random.fold_in(keys[4], 71), 0)
    embedding = draw_embedding(jax.random.fold_in(keys[4], 71), 0)
    targets = plant(skewed_wide(keys[2], (TOKENS,), VOCAB, 2), jax.random.fold_in(keys[2], 3), 0, VOCAB - 1).astype(jnp.int32)
    loss_weight = jnp.clip(jnp.exp(math.log(10.0) - 2.3025851 * jax.random.uniform(keys[3], (TOKENS,), jnp.float32) ** levels(keys[3], (TOKENS,), ((0, 8),), -0.2, 0.2)), 1.0, 10.0).astype(jnp.bfloat16)
    return dict(hidden=hidden, embedding=embedding, targets=targets, loss_weight=loss_weight)


soft_cap = 30.0
z_weight = 0.002


def capped_block(hidden, table_rows):
    logits = lax.dot_general(hidden, table_rows, (((1,), (1,)), ((), ())), preferred_element_type=jnp.float32)
    return soft_cap * jnp.tanh(logits / soft_cap)


def reference(hidden, embedding, targets, loss_weight):
    block_rows = VROWS * N_VOCAB
    table_blocks = embedding.reshape(VOCAB // block_rows, block_rows, D)

    def add_exp(exp_total, table_rows):
        capped = capped_block(hidden, table_rows)
        return exp_total + jnp.sum(jnp.exp(capped - soft_cap), axis=1), None

    exp_total, _ = lax.scan(add_exp, jnp.zeros((hidden.shape[0],), jnp.float32), table_blocks)
    weight = loss_weight.astype(jnp.float32)
    log_total = soft_cap + jnp.log(exp_total)
    factor = weight * (1.0 + 2.0 * z_weight * log_total) / exp_total

    def grads(accum_grad, blocks_item):
        table_rows, first_row = blocks_item
        capped = capped_block(hidden, table_rows)
        columns = first_row + jnp.arange(block_rows, dtype=jnp.int32)
        target_hit = targets[:, None] == columns[None, :]
        softmax_part = factor[:, None] * jnp.exp(capped - soft_cap) - jnp.where(target_hit, weight[:, None], 0.0)
        scores_grad = (softmax_part * (1.0 - (capped / soft_cap) ** 2)).astype(jnp.bfloat16)
        accum_grad = accum_grad + jnp.dot(scores_grad, table_rows, preferred_element_type=jnp.float32)
        rows_grad = lax.dot_general(scores_grad, hidden, (((0,), (0,)), ((), ())), preferred_element_type=jnp.float32)
        return accum_grad, rows_grad.astype(jnp.bfloat16)

    first_rows = jnp.arange(VOCAB // block_rows, dtype=jnp.int32) * block_rows
    hidden_sum, block_grads = lax.scan(grads, jnp.zeros(hidden.shape, jnp.float32), (table_blocks, first_rows))
    return hidden_sum.astype(jnp.bfloat16), block_grads.reshape(VOCAB, D)
```

```python
import functools

import jax
import jax.numpy as jnp
from jax import lax
from jax.experimental import pallas as pl
from jax.experimental.pallas import tpu as pltpu
from jax.sharding import Mesh
from jax.sharding import PartitionSpec as P

MESH = pl.DeviceIdType.MESH
f32, bf16 = jnp.float32, jnp.bfloat16

NY, NC, NX, NZ = 4, 2, 4, 8
D, VROWS, ROWS = 3584, 768, 64
TOKENS = ROWS * NY * NC
HALF = ROWS * NY
BLK = D // NX
SUB = ROWS // 2
ZR = ROWS // NZ
ORDER = (2, 1, 3, 0)

soft_cap = 30.0
z_weight = 0.002


def kernel(
    hid_in, emb_in, w_in, t_in, hg_out, tg_out,
    hid, emb, wtb, wrep, trep, logit, quad, sums, stat, stat2, stat3, frep, b1, b2, b3,
    sc, sct, own, dsend, drecv, xs, ry, rx, ys, xs2, sy, sx, zs, rz, gz, gx, stage,
    local_sem, send_sem, ra, rd, rw, rb, rdd, rsy, rsx, rty, rtx, rzs, rzg, rxg, tg_sem,
):
    y, c, x, z = (lax.axis_index(a) for a in ("y", "c", "x", "z"))
    rem = lax.rem

    def at(i, n):
        return rem(i + n, n)

    sends = []

    def start(src, dst, rsem, **dev):
        copy = pltpu.make_async_remote_copy(
            src_ref=src, dst_ref=dst, send_sem=send_sem.at[len(sends)], recv_sem=rsem, device_id=dev, device_id_type=MESH
        )
        copy.start()
        sends.append(copy)

    def arrived(dst, rsem):
        pltpu.make_async_remote_copy(
            src_ref=dst, dst_ref=dst, send_sem=send_sem.at[0], recv_sem=rsem, device_id={"c": 1 - c}, device_id_type=MESH
        ).wait_recv()

    def cols(q):
        return pl.ds(pl.multiple_of(q * BLK, 128), BLK)

    def piece(cc, yy, q):
        return hid.at[pl.ds(pl.multiple_of((cc * NY + yy) * ROWS, ROWS), ROWS), cols(q)]

    def shard(cc, yy):
        return hid.at[pl.ds(pl.multiple_of((cc * NY + yy) * ROWS, ROWS), ROWS)]

    load_own = pltpu.make_async_copy(hid_in, shard(c, y), local_sem.at[0])
    load_own.start()
    load_emb = []
    for k in range(NX):
        part = pl.ds(k * (VROWS // NX), VROWS // NX)
        load_emb.append(pltpu.make_async_copy(emb_in.at[part], emb.at[part], local_sem.at[1 + k]))
        load_emb[-1].start()

    barrier = pltpu.get_barrier_semaphore()
    yc_peers = [(dy, dc) for dy in range(NY) for dc in range(NC) if (dy, dc) != (0, 0)]
    for dy, dc in yc_peers:
        pl.semaphore_signal(barrier, inc=1, device_id={"y": at(y + dy, NY), "c": at(c + dc, NC)}, device_id_type=MESH)
    for d in range(1, NX):
        pl.semaphore_signal(barrier, inc=1, device_id={"x": at(x + d, NX)}, device_id_type=MESH)
    for d in range(1, NZ):
        pl.semaphore_signal(barrier, inc=1, device_id={"z": at(z + d, NZ)}, device_id_type=MESH)

    none = jnp.zeros((1, ROWS), f32)
    first = rem(y, 2) == 0
    me = c * NY + y
    rows2 = []
    for v in (w_in[...].astype(f32), t_in[...].astype(f32)):
        rows2.append(jnp.where(first, jnp.concatenate([v, none], 1), jnp.concatenate([none, v], 1)))
    wtb[me] = jnp.concatenate(rows2, 0)

    pl.semaphore_wait(barrier, len(yc_peers) + NX - 1 + NZ - 1)

    s0 = rem(x, 2) * 2
    s1 = s0 + 1
    o0 = 2 - s0
    o1 = o0 + 1
    up, down = at(y + 1, NY), at(y - 1, NY)
    far = at(y + 2, NY)
    right, left = at(x + 1, NX), at(x - 1, NX)
    MINUS, PLUS, FAR = 0, 1, 2
    load_own.wait()
    start(piece(c, y, s0), piece(c, y, s0), ra.at[MINUS * 4 + 0], y=up)
    start(piece(c, y, s1), piece(c, y, s1), ra.at[PLUS * 4 + 1], y=down)
    start(piece(c, y, s1), piece(c, y, s1), ra.at[MINUS * 4 + 1], y=up)
    start(piece(c, y, s0), piece(c, y, s0), ra.at[PLUS * 4 + 0], y=down)
    start(shard(c, y), shard(c, y), rd.at[12], c=1 - c)
    for k, (dy, dc) in enumerate(yc_peers):
        start(wtb.at[me], wtb.at[me], rw.at[k], y=at(y + dy, NY), c=at(c + dc, NC))

    where = {MINUS: down, PLUS: up, FAR: far}
    klass = (s0, s1, o0, o1)

    def got(src, k):
        p = piece(c, where[src], klass[k])
        arrived(p, ra.at[src * 4 + k])
        if k < 2 and src != FAR:
            if src == MINUS and k == 0:
                start(p, p, ra.at[FAR * 4 + 0], y=up)
            if src == PLUS and k == 1:
                start(p, p, ra.at[FAR * 4 + 1], y=down)
        if k == 0:
            start(p, p, ra.at[src * 4 + 2], x=left)
        if k == 1:
            start(p, p, ra.at[src * 4 + 3], x=right)
        start(p, p, rd.at[src * 4 + k], c=1 - c)

    def from_partner(k):
        for src in (MINUS, PLUS, FAR):
            arrived(piece(1 - c, where[src], klass[k]), rd.at[src * 4 + k])

    def add_logits(k, first_one):
        out = lax.dot_general(
            hid[:, cols(klass[k])], emb[:, cols(klass[k])], (((1,), (1,)), ((), ())), preferred_element_type=f32
        )
        logit[...] = out if first_one else logit[...] + out

    got(MINUS, 0)
    got(PLUS, 1)
    got(MINUS, 1)
    got(PLUS, 0)

    for k, (dy, dc) in enumerate(yc_peers):
        arrived(wtb.at[at(c - dc, NC) * NY + at(y - dy, NY)], rw.at[k])
    for b in range(TOKENS // 128):
        both = wtb[2 * b] + wtb[2 * b + 1]
        wrep[128 * b : 128 * b + 128, :] = jnp.broadcast_to(both[0:1, :], (128, 128)).T
        trep[128 * b : 128 * b + 128, :] = jnp.broadcast_to(both[1:2, :], (128, 128)).T

    got(MINUS, 2)
    got(PLUS, 3)
    got(FAR, 0)
    got(FAR, 1)
    for load in load_emb:
        load.wait()
    arrived(shard(1 - c, y), rd.at[12])
    got(PLUS, 2)
    got(MINUS, 3)
    from_partner(0)
    add_logits(0, True)
    got(FAR, 2)
    got(FAR, 3)
    from_partner(1)
    add_logits(1, False)
    from_partner(2)
    add_logits(2, False)
    from_partner(3)
    add_logits(3, False)

    def exps(i, carry):
        r = pl.ds(pl.multiple_of(i * 32, 32), 32)
        t = jnp.tanh(logit[r, :] * (1.0 / soft_cap))
        e = jnp.exp(soft_cap * t - soft_cap)
        logit[r, :] = e
        quad[r, :] = 1.0 - t * t
        total = e[:, 0:128]
        for k in range(1, VROWS // 128):
            total = total + e[:, 128 * k : 128 * k + 128]
        sums[r, :] = total
        return carry

    lax.fori_loop(0, TOKENS // 32, exps, 0)
    for b in range(TOKENS // 128):
        stat[0:1, 128 * b : 128 * b + 128] = jnp.sum(sums[128 * b : 128 * b + 128, :].T, axis=0, keepdims=True)

    for k, (dy, dc) in enumerate(yc_peers):
        start(stat, b1.at[k], rb.at[k], y=at(y + dy, NY), c=at(c + dc, NC))
    n1 = len(yc_peers)
    for k in range(n1):
        arrived(b1.at[k], rb.at[k])
    total = stat[...]
    for k in range(n1):
        total = total + b1[k]
    stat2[...] = total
    for d in range(1, NX):
        start(stat2, b2.at[d - 1], rb.at[n1 + d - 1], x=at(x + d, NX))
    for d in range(1, NX):
        arrived(b2.at[d - 1], rb.at[n1 + d - 1])
    for d in range(1, NX):
        total = total + b2[d - 1]
    stat3[...] = total
    n2 = n1 + NX - 1
    for d in range(1, NZ):
        start(stat3, b3.at[d - 1], rb.at[n2 + d - 1], z=at(z + d, NZ))
    for d in range(1, NZ):
        arrived(b3.at[d - 1], rb.at[n2 + d - 1])
    for d in range(1, NZ):
        total = total + b3[d - 1]
    rate = (1.0 + 2.0 * z_weight * (soft_cap + jnp.log(total))) / total
    for b in range(TOKENS // 128):
        frep[128 * b : 128 * b + 128, :] = jnp.broadcast_to(rate[0:1, 128 * b : 128 * b + 128], (128, 128)).T

    base = ((((y * NC + c) * NX + x) * NZ + z) * VROWS).astype(f32)

    def scores(i, carry):
        r = pl.ds(pl.multiple_of(i * 32, 32), 32)
        w = wrep[r, :]
        fac = frep[r, :] * w
        want = trep[r, :] - base
        lane = lax.broadcasted_iota(jnp.int32, (32, 128), 1).astype(f32)
        for k in range(VROWS // 128):
            s = slice(128 * k, 128 * k + 128)
            hit = jnp.where(want == lane + float(128 * k), w, 0.0)
            sc[r, s] = ((fac * logit[r, s] - hit) * quad[r, s]).astype(bf16)
        return carry

    lax.fori_loop(0, TOKENS // 32, scores, 0)

    other_rows = pl.ds(pl.multiple_of((1 - c) * HALF, HALF), HALF)
    own_rows = pl.ds(pl.multiple_of(c * HALF, HALF), HALF)
    blocks = [at(x + d, NX) for d in ORDER]
    for i in range(NX):
        e = emb[:, cols(blocks[i])]
        dsend[i] = jnp.dot(sc[other_rows, :], e, preferred_element_type=f32).astype(bf16)
        start(dsend.at[i], drecv.at[i], rdd.at[i], c=1 - c)
        own[i] = jnp.dot(sc[own_rows, :], e, preferred_element_type=f32)
    for i, d in enumerate(ORDER):
        arrived(drecv.at[i], rdd.at[i])
        chip = own[i] + drecv[i].astype(f32)
        own[i] = chip
        xs[i] = chip.astype(bf16).reshape(NY, 2, SUB, BLK)
        for dy in (2, 1, 3):
            yy = at(y + dy, NY)
            start(xs.at[i, yy, 0], ry.at[dy - 1, i], rsy.at[(dy - 1) * NX + i], y=yy)
        if d:
            start(xs.at[i, :, 1], rx.at[d - 1], rsx.at[d - 1], x=blocks[i])

    for k in range(VROWS // 128):
        s = slice(128 * k, 128 * k + 128)
        sct[s, :] = sc[:, s].astype(f32).T.astype(bf16)
    outs = []
    for i in range(NX):
        stage[i] = jnp.dot(sct[...], hid[:, i * BLK : (i + 1) * BLK], preferred_element_type=f32).astype(bf16)
        outs.append(pltpu.make_async_copy(stage.at[i], tg_out.at[:, i * BLK : (i + 1) * BLK], tg_sem.at[i]))
        outs[-1].start()

    def own_part(i, yy, colour):
        return own[i, pl.ds(pl.multiple_of(yy * ROWS + colour * SUB, SUB), SUB), :]

    for i, d in enumerate(ORDER):
        total = own_part(i, y, 0)
        for dy in range(1, NY):
            arrived(ry.at[dy - 1, i], rsy.at[(dy - 1) * NX + i])
            total = total + ry[dy - 1, i].astype(f32)
        if d:
            ys[d - 1] = total.astype(bf16)
            start(ys.at[d - 1], sy.at[d - 1], rty.at[d - 1], x=blocks[i])
        else:
            keep0 = total
    for d in range(1, NX):
        arrived(rx.at[d - 1], rsx.at[d - 1])
    mine = ORDER.index(0)

    def x_sum(yy):
        total = own_part(mine, yy, 1)
        for d in range(1, NX):
            total = total + rx[d - 1, yy].astype(f32)
        return total

    for dy in (2, 1, 3):
        yy = at(y + dy, NY)
        xs2[dy - 1] = x_sum(yy).astype(bf16)
        start(xs2.at[dy - 1], sx.at[dy - 1], rtx.at[dy - 1], y=yy)
    keep1 = x_sum(y)
    for d in range(1, NX):
        arrived(sy.at[d - 1], rty.at[d - 1])
        keep0 = keep0 + sy[d - 1].astype(f32)
    for d in range(1, NY):
        arrived(sx.at[d - 1], rtx.at[d - 1])
        keep1 = keep1 + sx[d - 1].astype(f32)

    half = NZ // 2
    zs[0:half] = keep0.reshape(half, ZR, BLK)
    zs[half:NZ] = keep1.reshape(half, ZR, BLK)
    for d in (4, 3, 5, 2, 6, 1, 7):
        zz = at(z + d, NZ)
        start(zs.at[zz], rz.at[d - 1], rzs.at[d - 1], z=zz)
    total = zs[z]
    for d in range(1, NZ):
        arrived(rz.at[d - 1], rzs.at[d - 1])
        total = total + rz[d - 1]
    gz[z] = total.astype(bf16)
    for d in (4, 3, 5, 2, 6, 1, 7):
        start(gz.at[z], gz.at[z], rzg.at[d - 1], z=at(z + d, NZ))
    for d in range(1, NZ):
        arrived(gz.at[at(z - d, NZ)], rzg.at[d - 1])
    for d in (2, 1, 3):
        start(gz, gx.at[d - 1], rxg.at[d - 1], x=at(x + d, NX))
    hg_out[:, cols(x)] = gz[...].reshape(ROWS, BLK)
    for d in range(1, NX):
        arrived(gx.at[d - 1], rxg.at[d - 1])
        hg_out[:, cols(at(x - d, NX))] = gx[d - 1].reshape(ROWS, BLK)

    for out in outs:
        out.wait()
    for copy in sends:
        copy.wait_send()


def body(hidden, embedding, targets, loss_weight):
    vm = pltpu.VMEM
    dma = pltpu.SemaphoreType.DMA
    return pl.pallas_call(
        kernel,
        out_shape=(
            jax.ShapeDtypeStruct((ROWS, D), bf16),
            jax.ShapeDtypeStruct((VROWS, D), bf16),
        ),
        in_specs=[
            pl.BlockSpec(memory_space=pl.ANY),
            pl.BlockSpec(memory_space=pl.ANY),
            pl.BlockSpec(memory_space=pltpu.VMEM),
            pl.BlockSpec(memory_space=pltpu.VMEM),
        ],
        out_specs=(pl.BlockSpec(memory_space=pltpu.VMEM), pl.BlockSpec(memory_space=pl.ANY)),
        scratch_shapes=[
            vm((TOKENS, D), bf16),
            vm((VROWS, D), bf16),
            vm((NC * NY, 2, 128), f32),
            vm((TOKENS, 128), f32),
            vm((TOKENS, 128), f32),
            vm((TOKENS, VROWS), f32),
            vm((TOKENS, VROWS), f32),
            vm((TOKENS, 128), f32),
            vm((1, TOKENS), f32),
            vm((1, TOKENS), f32),
            vm((1, TOKENS), f32),
            vm((TOKENS, 128), f32),
            vm((NY * NC - 1, 1, TOKENS), f32),
            vm((NX - 1, 1, TOKENS), f32),
            vm((NZ - 1, 1, TOKENS), f32),
            vm((TOKENS, VROWS), bf16),
            vm((VROWS, TOKENS), bf16),
            vm((NX, HALF, BLK), f32),
            vm((NX, HALF, BLK), bf16),
            vm((NX, HALF, BLK), bf16),
            vm((NX, NY, 2, SUB, BLK), bf16),
            vm((NY - 1, NX, SUB, BLK), bf16),
            vm((NX - 1, NY, SUB, BLK), bf16),
            vm((NX - 1, SUB, BLK), bf16),
            vm((NY - 1, SUB, BLK), bf16),
            vm((NX - 1, SUB, BLK), bf16),
            vm((NY - 1, SUB, BLK), bf16),
            vm((NZ, ZR, BLK), f32),
            vm((NZ - 1, ZR, BLK), f32),
            vm((NZ, ZR, BLK), bf16),
            vm((NX - 1, NZ, ZR, BLK), bf16),
            vm((NX, VROWS, BLK), bf16),
            dma((1 + NX,)),
            dma((104,)),
            dma((12,)),
            dma((13,)),
            dma((NY * NC - 1,)),
            dma((NY * NC + NX + NZ - 3,)),
            dma((NX,)),
            dma(((NY - 1) * NX,)),
            dma((NX - 1,)),
            dma((NX - 1,)),
            dma((NY - 1,)),
            dma((NZ - 1,)),
            dma((NZ - 1,)),
            dma((NX - 1,)),
            dma((NX,)),
        ],
        compiler_params=pltpu.CompilerParams(collective_id=0, has_side_effects=True, vmem_limit_bytes=60 * 1024 * 1024),
        name="head_backward",
    )(hidden, embedding, loss_weight.reshape(1, ROWS), targets.reshape(1, ROWS))


def solution(mesh):
    finer = Mesh(mesh.devices.reshape(NY, NC, NX, NZ), ("y", "c", "x", "z"))
    dp = ("y", "c")
    both = ("y", "c", "x", "z")
    return jax.shard_map(
        body,
        mesh=finer,
        in_specs=(P(dp, None), P(both, None), P(dp), P(dp)),
        out_specs=(P(dp, None), P(both, None)),
        check_vma=False,
    )
```

```python
import functools

import jax
import jax.numpy as jnp
from jax import lax
from jax.experimental import pallas as pl
from jax.experimental.pallas import tpu as pltpu
from jax.sharding import Mesh
from jax.sharding import PartitionSpec as P

MESH = pl.DeviceIdType.MESH
f32, bf16 = jnp.float32, jnp.bfloat16

NY, NC, NX, NZ = 4, 2, 4, 8
D, VROWS, ROWS = 3584, 768, 64
TOKENS = ROWS * NY * NC
HALF = ROWS * NY
BLK = D // NX
SUB = ROWS // 2
ZR = ROWS // NZ
ORDER = (2, 1, 3, 0)

soft_cap = 30.0
z_weight = 0.002


def kernel(
    hid_in, emb_in, w_in, t_in, hg_out, tg_out,
    w_own, t_own, hid, emb, wtb, wrep, trep, logit, quad, sums, stat, stat2, stat3, frep, b1, b2, b3,
    sc, sct, own, dsend, drecv, xs, ry, rx, ys, xs2, sy, sx, zf, zs, rz, gz, gx,
    local_sem, send_sem, ra, rd, rw, rb, rdd, rsy, rsx, rty, rtx, rzs, rzg, rxg,
):
    y, c, x, z = (lax.axis_index(a) for a in ("y", "c", "x", "z"))
    rem = lax.rem

    def at(i, n):
        return rem(i + n, n)

    sends = []

    def start(src, dst, rsem, **dev):
        copy = pltpu.make_async_remote_copy(
            src_ref=src, dst_ref=dst, send_sem=send_sem.at[len(sends)], recv_sem=rsem, device_id=dev, device_id_type=MESH
        )
        copy.start()
        sends.append(copy)

    def arrived(dst, rsem):
        pltpu.make_async_remote_copy(
            src_ref=dst, dst_ref=dst, send_sem=send_sem.at[0], recv_sem=rsem, device_id={"c": 1 - c}, device_id_type=MESH
        ).wait_recv()

    me = c * NY + y

    def cols(q):
        return pl.ds(pl.multiple_of(q * BLK, 128), BLK)

    def shard(cc, yy):
        return hid.at[pl.ds(pl.multiple_of((cc * NY + yy) * ROWS, ROWS), ROWS)]

    def piece(cc, yy, q, lo, hi):
        rows = pl.ds(pl.multiple_of((cc * NY + yy) * ROWS, ROWS), ROWS)
        return hid.at[rows, pl.ds(pl.multiple_of(q * BLK + lo, 128), hi - lo)]

    load_own = [
        pltpu.make_async_copy(hid_in, shard(c, y), local_sem.at[NX]),
        pltpu.make_async_copy(w_in, w_own, local_sem.at[NX + 1]),
        pltpu.make_async_copy(t_in, t_own, local_sem.at[NX + 2]),
    ]
    load_emb = []
    for k in range(NX):
        part = pl.ds(k * (VROWS // NX), VROWS // NX)
        load_emb.append(pltpu.make_async_copy(emb_in.at[part], emb.at[part], local_sem.at[k]))
    for load in load_own + load_emb:
        load.start()

    barrier = pltpu.get_barrier_semaphore()
    yc_peers = [(dy, dc) for dy in range(NY) for dc in range(NC) if (dy, dc) != (0, 0)]
    for dy, dc in yc_peers:
        pl.semaphore_signal(barrier, inc=1, device_id={"y": at(y + dy, NY), "c": at(c + dc, NC)}, device_id_type=MESH)
    for d in range(1, NX):
        pl.semaphore_signal(barrier, inc=1, device_id={"x": at(x + d, NX)}, device_id_type=MESH)
    for d in range(1, NZ):
        pl.semaphore_signal(barrier, inc=1, device_id={"z": at(z + d, NZ)}, device_id_type=MESH)

    for load in load_own:
        load.wait()
    none = jnp.zeros((1, ROWS), f32)
    first = rem(y, 2) == 0
    rows2 = []
    for v in (w_own[...].astype(f32), t_own[...].astype(f32)):
        rows2.append(jnp.where(first, jnp.concatenate([v, none], 1), jnp.concatenate([none, v], 1)))
    wtb[me] = jnp.concatenate(rows2, 0)

    pl.semaphore_wait(barrier, len(yc_peers) + NX - 1 + NZ - 1)

    k0 = rem(x + 2 * z, NX)
    kp, km, k2 = rem(k0 + 1, NX), rem(k0 + 3, NX), rem(k0 + 2, NX)
    up, down, far = at(y + 1, NY), at(y - 1, NY), at(y + 2, NY)
    right, left = at(x + 1, NX), at(x - 1, NX)
    above, below = at(z + 1, NZ), at(z - 1, NZ)
    MINUS, PLUS, FAR = 0, 1, 2
    where = {MINUS: down, PLUS: up, FAR: far}
    P1, P2, P3, P4, R1, R2, L1, L2, ZU, ZD = range(10)
    parts = (
        (k0, 0, 512), (k0, 512, BLK), (kp, 0, 256), (km, 0, 256),
        (kp, 256, 512), (kp, 512, BLK), (km, 256, 512), (km, 512, BLK),
        (k2, 0, 512), (k2, 512, BLK),
    )
    NP = len(parts)

    def own_to(p, src, yy):
        part = piece(c, y, *parts[p])
        start(part, part, ra.at[src * NP + p], y=yy)

    for p, q in ((P1, P2), (P3, P4), (P2, P1), (P4, P3)):
        own_to(p, MINUS, up)
        own_to(q, PLUS, down)
    start(shard(c, y), shard(c, y), rd.at[3 * NP], c=1 - c)
    for k, (dy, dc) in enumerate(yc_peers):
        start(wtb.at[me], wtb.at[me], rw.at[k], y=at(y + dy, NY), c=at(c + dc, NC))

    def got(src, p):
        part = piece(c, where[src], *parts[p])
        arrived(part, ra.at[src * NP + p])
        if src == MINUS and p in (P1, P3):
            start(part, part, ra.at[FAR * NP + p], y=up)
        if src == PLUS and p in (P2, P4):
            start(part, part, ra.at[FAR * NP + p], y=down)
        if p in (P1, P2):
            sub = piece(c, where[src], k0, 256, 512) if p == P1 else part
            start(sub, sub, ra.at[src * NP + (R1 if p == P1 else R2)], x=left)
            start(sub, sub, ra.at[src * NP + (L1 if p == P1 else L2)], x=right)
            if p == P1:
                start(part, part, ra.at[src * NP + ZU], z=below)
            else:
                start(part, part, ra.at[src * NP + ZD], z=above)
        start(part, part, rd.at[src * NP + p], c=1 - c)

    def from_partner(*ps):
        for p in ps:
            for src in (MINUS, PLUS, FAR):
                arrived(piece(1 - c, where[src], *parts[p]), rd.at[src * NP + p])

    def add_logits(q, first_one):
        out = lax.dot_general(
            hid[:, cols(q)], emb[:, cols(q)], (((1,), (1,)), ((), ())), preferred_element_type=f32
        )
        logit[...] = out if first_one else logit[...] + out

    for src, p in ((PLUS, P2), (MINUS, P1), (PLUS, P4), (MINUS, P3), (MINUS, P2), (PLUS, P1)):
        got(src, p)

    for k, (dy, dc) in enumerate(yc_peers):
        arrived(wtb.at[at(c - dc, NC) * NY + at(y - dy, NY)], rw.at[k])
    for b in range(TOKENS // 128):
        both = wtb[2 * b] + wtb[2 * b + 1]
        wrep[128 * b : 128 * b + 128, :] = jnp.broadcast_to(both[0:1, :], (128, 128)).T
        trep[128 * b : 128 * b + 128, :] = jnp.broadcast_to(both[1:2, :], (128, 128)).T

    for src, p in (
        (MINUS, P4), (PLUS, P3), (PLUS, R2), (PLUS, L2), (PLUS, ZD), (MINUS, R1), (MINUS, L1), (MINUS, ZU),
        (FAR, P2), (FAR, P1), (FAR, P4), (FAR, P3), (MINUS, R2), (MINUS, L2), (MINUS, ZD), (PLUS, ZU),
        (PLUS, R1), (PLUS, L1),
    ):
        got(src, p)
    for load in load_emb:
        load.wait()
    arrived(shard(1 - c, y), rd.at[3 * NP])
    from_partner(P1, P2)
    add_logits(k0, True)
    for p in (R2, L2, ZD, R1, L1, ZU):
        got(FAR, p)
    from_partner(P3, R2, R1)
    add_logits(kp, False)
    from_partner(P4, L2, L1)
    add_logits(km, False)
    from_partner(ZD, ZU)
    add_logits(k2, False)

    def exps(i, carry):
        r = pl.ds(pl.multiple_of(i * 32, 32), 32)
        t = jnp.tanh(logit[r, :] * (1.0 / soft_cap))
        e = jnp.exp(soft_cap * t - soft_cap)
        logit[r, :] = e
        quad[r, :] = 1.0 - t * t
        total = e[:, 0:128]
        for k in range(1, VROWS // 128):
            total = total + e[:, 128 * k : 128 * k + 128]
        sums[r, :] = total
        return carry

    lax.fori_loop(0, TOKENS // 32, exps, 0)
    for b in range(TOKENS // 128):
        stat[0:1, 128 * b : 128 * b + 128] = jnp.sum(sums[128 * b : 128 * b + 128, :].T, axis=0, keepdims=True)

    for k, (dy, dc) in enumerate(yc_peers):
        start(stat, b1.at[k], rb.at[k], y=at(y + dy, NY), c=at(c + dc, NC))
    n1 = len(yc_peers)
    for k in range(n1):
        arrived(b1.at[k], rb.at[k])
    total = stat[...]
    for k in range(n1):
        total = total + b1[k]
    stat2[...] = total
    for d in range(1, NX):
        start(stat2, b2.at[d - 1], rb.at[n1 + d - 1], x=at(x + d, NX))
    for d in range(1, NX):
        arrived(b2.at[d - 1], rb.at[n1 + d - 1])
    for d in range(1, NX):
        total = total + b2[d - 1]
    stat3[...] = total
    n2 = n1 + NX - 1
    for d in range(1, NZ):
        start(stat3, b3.at[d - 1], rb.at[n2 + d - 1], z=at(z + d, NZ))
    for d in range(1, NZ):
        arrived(b3.at[d - 1], rb.at[n2 + d - 1])
    for d in range(1, NZ):
        total = total + b3[d - 1]
    rate = (1.0 + 2.0 * z_weight * (soft_cap + jnp.log(total))) / total
    for b in range(TOKENS // 128):
        frep[128 * b : 128 * b + 128, :] = jnp.broadcast_to(rate[0:1, 128 * b : 128 * b + 128], (128, 128)).T

    base = ((((y * NC + c) * NX + x) * NZ + z) * VROWS).astype(f32)

    def scores(i, carry):
        r = pl.ds(pl.multiple_of(i * 32, 32), 32)
        w = wrep[r, :]
        fac = frep[r, :] * w
        want = trep[r, :] - base
        lane = lax.broadcasted_iota(jnp.int32, (32, 128), 1).astype(f32)
        for k in range(VROWS // 128):
            s = slice(128 * k, 128 * k + 128)
            hit = jnp.where(want == lane + float(128 * k), w, 0.0)
            sc[r, s] = ((fac * logit[r, s] - hit) * quad[r, s]).astype(bf16)
        return carry

    lax.fori_loop(0, TOKENS // 32, scores, 0)

    other_rows = pl.ds(pl.multiple_of((1 - c) * HALF, HALF), HALF)
    own_rows = pl.ds(pl.multiple_of(c * HALF, HALF), HALF)
    blocks = [at(x + d, NX) for d in ORDER]
    for i in range(NX):
        e = emb[:, cols(blocks[i])]
        dsend[i] = jnp.dot(sc[other_rows, :], e, preferred_element_type=f32).astype(bf16)
        start(dsend.at[i], drecv.at[i], rdd.at[i], c=1 - c)
        own[i] = jnp.dot(sc[own_rows, :], e, preferred_element_type=f32)
    for i, d in enumerate(ORDER):
        arrived(drecv.at[i], rdd.at[i])
        chip = own[i] + drecv[i].astype(f32)
        own[i] = chip
        xs[i] = chip.astype(bf16).reshape(NY, 2, SUB, BLK)
        for dy in (2, 1, 3):
            yy = at(y + dy, NY)
            start(xs.at[i, yy, 0], ry.at[dy - 1, i], rsy.at[(dy - 1) * NX + i], y=yy)
        if d:
            start(xs.at[i, :, 1], rx.at[d - 1], rsx.at[d - 1], x=blocks[i])

    for k in range(VROWS // 128):
        s = slice(128 * k, 128 * k + 128)
        sct[s, :] = sc[:, s].astype(f32).T.astype(bf16)
    for i in range(NX):
        tg_out[:, i * BLK : (i + 1) * BLK] = jnp.dot(
            sct[...], hid[:, i * BLK : (i + 1) * BLK], preferred_element_type=f32
        ).astype(bf16)

    def own_part(i, yy, colour):
        return own[i, pl.ds(pl.multiple_of(yy * ROWS + colour * SUB, SUB), SUB), :]

    for i, d in enumerate(ORDER):
        total = own_part(i, y, 0)
        for dy in range(1, NY):
            arrived(ry.at[dy - 1, i], rsy.at[(dy - 1) * NX + i])
            total = total + ry[dy - 1, i].astype(f32)
        if d:
            ys[d - 1] = total.astype(bf16)
            start(ys.at[d - 1], sy.at[d - 1], rty.at[d - 1], x=blocks[i])
        else:
            keep0 = total
    for d in range(1, NX):
        arrived(rx.at[d - 1], rsx.at[d - 1])
    mine = ORDER.index(0)

    def x_sum(yy):
        total = own_part(mine, yy, 1)
        for d in range(1, NX):
            total = total + rx[d - 1, yy].astype(f32)
        return total

    for dy in (2, 1, 3):
        yy = at(y + dy, NY)
        xs2[dy - 1] = x_sum(yy).astype(bf16)
        start(xs2.at[dy - 1], sx.at[dy - 1], rtx.at[dy - 1], y=yy)
    keep1 = x_sum(y)
    for d in range(1, NX):
        arrived(sy.at[d - 1], rty.at[d - 1])
        keep0 = keep0 + sy[d - 1].astype(f32)
    for d in range(1, NY):
        arrived(sx.at[d - 1], rtx.at[d - 1])
        keep1 = keep1 + sx[d - 1].astype(f32)

    half = NZ // 2
    zf[0:half] = keep0.reshape(half, ZR, BLK)
    zf[half:NZ] = keep1.reshape(half, ZR, BLK)
    zs[...] = zf[...].astype(bf16)
    for d in (4, 3, 5, 2, 6, 1, 7):
        zz = at(z + d, NZ)
        start(zs.at[zz], rz.at[d - 1], rzs.at[d - 1], z=zz)
    total = zf[z]
    for d in (1, 7, 2, 6, 3, 5, 4):
        arrived(rz.at[d - 1], rzs.at[d - 1])
        total = total + rz[d - 1].astype(f32)
    gz[z] = total.astype(bf16)
    for d in (4, 3, 5, 2, 6, 1, 7):
        start(gz.at[z], gz.at[z], rzg.at[d - 1], z=at(z + d, NZ))

    def on_to_x(d, zz):
        for dx in (2, 1, 3):
            start(gz.at[zz], gx.at[dx - 1, zz], rxg.at[(dx - 1) * NZ + d], x=at(x + dx, NX))

    on_to_x(0, z)
    for d in (1, 7, 2, 6, 3, 5, 4):
        arrived(gz.at[at(z - d, NZ)], rzg.at[d - 1])
        on_to_x(d, at(z - d, NZ))
    hg_out[:, cols(x)] = gz[...].reshape(ROWS, BLK)
    for dx in range(1, NX):
        for d in range(NZ):
            arrived(gx.at[dx - 1, at(z - d, NZ)], rxg.at[(dx - 1) * NZ + d])
        hg_out[:, cols(at(x - dx, NX))] = gx[dx - 1].reshape(ROWS, BLK)

    for copy in sends:
        copy.wait_send()


def body(hidden, embedding, targets, loss_weight):
    vm = pltpu.VMEM
    dma = pltpu.SemaphoreType.DMA
    return pl.pallas_call(
        kernel,
        out_shape=(
            jax.ShapeDtypeStruct((ROWS, D), bf16),
            jax.ShapeDtypeStruct((VROWS, D), bf16),
        ),
        in_specs=[
            pl.BlockSpec(memory_space=pl.ANY),
            pl.BlockSpec(memory_space=pl.ANY),
            pl.BlockSpec(memory_space=pl.ANY),
            pl.BlockSpec(memory_space=pl.ANY),
        ],
        out_specs=(pl.BlockSpec(memory_space=pltpu.VMEM), pl.BlockSpec(memory_space=pltpu.VMEM)),
        scratch_shapes=[
            vm((1, ROWS), bf16),
            vm((1, ROWS), jnp.int32),
            vm((TOKENS, D), bf16),
            vm((VROWS, D), bf16),
            vm((NC * NY, 2, 128), f32),
            vm((TOKENS, 128), f32),
            vm((TOKENS, 128), f32),
            vm((TOKENS, VROWS), f32),
            vm((TOKENS, VROWS), f32),
            vm((TOKENS, 128), f32),
            vm((1, TOKENS), f32),
            vm((1, TOKENS), f32),
            vm((1, TOKENS), f32),
            vm((TOKENS, 128), f32),
            vm((NY * NC - 1, 1, TOKENS), f32),
            vm((NX - 1, 1, TOKENS), f32),
            vm((NZ - 1, 1, TOKENS), f32),
            vm((TOKENS, VROWS), bf16),
            vm((VROWS, TOKENS), bf16),
            vm((NX, HALF, BLK), f32),
            vm((NX, HALF, BLK), bf16),
            vm((NX, HALF, BLK), bf16),
            vm((NX, NY, 2, SUB, BLK), bf16),
            vm((NY - 1, NX, SUB, BLK), bf16),
            vm((NX - 1, NY, SUB, BLK), bf16),
            vm((NX - 1, SUB, BLK), bf16),
            vm((NY - 1, SUB, BLK), bf16),
            vm((NX - 1, SUB, BLK), bf16),
            vm((NY - 1, SUB, BLK), bf16),
            vm((NZ, ZR, BLK), f32),
            vm((NZ, ZR, BLK), bf16),
            vm((NZ - 1, ZR, BLK), bf16),
            vm((NZ, ZR, BLK), bf16),
            vm((NX - 1, NZ, ZR, BLK), bf16),
            dma((NX + 3,)),
            dma((160,)),
            dma((30,)),
            dma((31,)),
            dma((NY * NC - 1,)),
            dma((NY * NC + NX + NZ - 3,)),
            dma((NX,)),
            dma(((NY - 1) * NX,)),
            dma((NX - 1,)),
            dma((NX - 1,)),
            dma((NY - 1,)),
            dma((NZ - 1,)),
            dma((NZ - 1,)),
            dma(((NX - 1) * NZ,)),
        ],
        compiler_params=pltpu.CompilerParams(collective_id=0, has_side_effects=True, vmem_limit_bytes=44 * 1024 * 1024),
        name="head_backward",
    )(*(pltpu.with_memory_space_constraint(a, pltpu.HBM) for a in (hidden, embedding, loss_weight.reshape(1, ROWS), targets.reshape(1, ROWS))))


def solution(mesh):
    finer = Mesh(mesh.devices.reshape(NY, NC, NX, NZ), ("y", "c", "x", "z"))
    dp = ("y", "c")
    both = ("y", "c", "x", "z")
    return jax.shard_map(
        body,
        mesh=finer,
        in_specs=(P(dp, None), P(both, None), P(dp), P(dp)),
        out_specs=(P(dp, None), P(both, None)),
        check_vma=False,
    )
```

```python
import functools

import jax
import jax.numpy as jnp
from jax import lax
from jax.experimental import pallas as pl
from jax.experimental.pallas import tpu as pltpu
from jax.sharding import Mesh
from jax.sharding import PartitionSpec as P

MESH = pl.DeviceIdType.MESH
f32, bf16 = jnp.float32, jnp.bfloat16

NY, NC, NX, NZ = 4, 2, 4, 8
D, VROWS, ROWS = 3584, 768, 64
TOKENS = ROWS * NY * NC
HALF = ROWS * NY
BLK = D // NX
SUB = ROWS // 2
ZR = ROWS // NZ
ORDER = (2, 1, 3, 0)

soft_cap = 30.0
z_weight = 0.002


def kernel(
    hid_in, emb_in, w_in, t_in, hg_out, tg_out,
    w_own, t_own, hid, emb, wtb, wrep, trep, prob, sums, hits, stat, stat2, stat3, rate, frep, grep, b1, b2, b3,
    pm, hm, sc, sct, own, town, asend, arecv, tsend, trecv, fy, fyr, ny, nyr, fx, fxr, nx, nxr,
    ys, xs2, sy, sx, zf, zs, rz, gz, gx,
    local_sem, send_sem, ra, rd, rw, rb, rda, rdt, rfy, rny, rfx, rnx, rty, rtx, rzs, rzg, rxg,
):
    y, c, x, z = (lax.axis_index(a) for a in ("y", "c", "x", "z"))
    rem = lax.rem

    def at(i, n):
        return rem(i + n, n)

    up, down, far = at(y + 1, NY), at(y - 1, NY), at(y + 2, NY)
    right, left = at(x + 1, NX), at(x - 1, NX)
    above, below = at(z + 1, NZ), at(z - 1, NZ)
    OWN, PLUS, MINUS, FAR = range(4)
    where = {OWN: y, PLUS: up, MINUS: down, FAR: far}
    RHO = ((0, OWN), (0, PLUS), (0, MINUS), (0, FAR), (1, FAR), (1, OWN), (1, PLUS), (1, MINUS))
    row_of = {key: ROWS * k for k, key in enumerate(RHO)}
    me = c * NY + y

    def group(e, s):
        return (1 - c if e else c) * NY + where[s]

    sends = []

    def start(src, dst, rsem, **dev):
        copy = pltpu.make_async_remote_copy(
            src_ref=src, dst_ref=dst, send_sem=send_sem.at[len(sends)], recv_sem=rsem, device_id=dev, device_id_type=MESH
        )
        copy.start()
        sends.append(copy)

    def arrived(dst, rsem):
        pltpu.make_async_remote_copy(
            src_ref=dst, dst_ref=dst, send_sem=send_sem.at[0], recv_sem=rsem, device_id={"c": 1 - c}, device_id_type=MESH
        ).wait_recv()

    def cols(q):
        return pl.ds(pl.multiple_of(q * BLK, 128), BLK)

    def shard(e, s):
        return hid.at[row_of[e, s] : row_of[e, s] + ROWS]

    def piece(e, s, q, lo, hi):
        return hid.at[row_of[e, s] : row_of[e, s] + ROWS, pl.ds(pl.multiple_of(q * BLK + lo, 128), hi - lo)]

    load_own = [
        pltpu.make_async_copy(hid_in, shard(0, OWN), local_sem.at[NX]),
        pltpu.make_async_copy(w_in, w_own, local_sem.at[NX + 1]),
        pltpu.make_async_copy(t_in, t_own, local_sem.at[NX + 2]),
    ]
    load_emb = []
    for k in range(NX):
        part = pl.ds(k * (VROWS // NX), VROWS // NX)
        load_emb.append(pltpu.make_async_copy(emb_in.at[part], emb.at[part], local_sem.at[k]))
    for load in load_own + load_emb:
        load.start()

    barrier = pltpu.get_barrier_semaphore()
    yc_peers = [(dy, dc) for dy in range(NY) for dc in range(NC) if (dy, dc) != (0, 0)]
    for dy, dc in yc_peers:
        pl.semaphore_signal(barrier, inc=1, device_id={"y": at(y + dy, NY), "c": at(c + dc, NC)}, device_id_type=MESH)
    for d in range(1, NX):
        pl.semaphore_signal(barrier, inc=1, device_id={"x": at(x + d, NX)}, device_id_type=MESH)
    for d in range(1, NZ):
        pl.semaphore_signal(barrier, inc=1, device_id={"z": at(z + d, NZ)}, device_id_type=MESH)

    for load in load_own:
        load.wait()
    none = jnp.zeros((1, ROWS), f32)
    wtb[me] = jnp.concatenate(
        [jnp.concatenate([v, none], 1) for v in (w_own[...].astype(f32), t_own[...].astype(f32))], 0
    )

    pl.semaphore_wait(barrier, len(yc_peers) + NX - 1 + NZ - 1)

    k0 = rem(x + 2 * z, NX)
    kp, km, k2 = rem(k0 + 1, NX), rem(k0 + 3, NX), rem(k0 + 2, NX)
    P1, P2, P3, P4, R1, R2, L1, L2, ZU, ZD = range(10)
    parts = (
        (k0, 0, 512), (k0, 512, BLK), (kp, 0, 256), (km, 0, 256),
        (kp, 256, 512), (kp, 512, BLK), (km, 256, 512), (km, 512, BLK),
        (k2, 0, 512), (k2, 512, BLK),
    )
    NP = len(parts)

    def slot(s, p):
        return (s - 1) * NP + p

    def to_up(s, p):
        start(piece(0, s, *parts[p]), piece(0, MINUS if s == OWN else FAR, *parts[p]), ra.at[slot(MINUS if s == OWN else FAR, p)], y=up)

    def to_down(s, p):
        start(piece(0, s, *parts[p]), piece(0, PLUS if s == OWN else FAR, *parts[p]), ra.at[slot(PLUS if s == OWN else FAR, p)], y=down)

    for p, q in ((P1, P2), (P3, P4), (P2, P1), (P4, P3)):
        to_up(OWN, p)
        to_down(OWN, q)
    start(shard(0, OWN), shard(1, OWN), rd.at[3 * NP], c=1 - c)
    for k, (dy, dc) in enumerate(yc_peers):
        start(wtb.at[me], wtb.at[me], rw.at[k], y=at(y + dy, NY), c=at(c + dc, NC))

    def got(s, p):
        part = piece(0, s, *parts[p])
        arrived(part, ra.at[slot(s, p)])
        if s == MINUS and p in (P1, P3):
            to_up(s, p)
        if s == PLUS and p in (P2, P4):
            to_down(s, p)
        if p in (P1, P2):
            sub = piece(0, s, k0, 256, 512) if p == P1 else part
            start(sub, sub, ra.at[slot(s, R1 if p == P1 else R2)], x=left)
            start(sub, sub, ra.at[slot(s, L1 if p == P1 else L2)], x=right)
            if p == P1:
                start(part, part, ra.at[slot(s, ZU)], z=below)
            else:
                start(part, part, ra.at[slot(s, ZD)], z=above)
        start(part, piece(1, s, *parts[p]), rd.at[slot(s, p)], c=1 - c)

    def from_partner(*ss):
        for s in ss:
            for p in range(NP):
                arrived(piece(1, s, *parts[p]), rd.at[slot(s, p)])

    def logits(lo, hi):
        prob[lo:hi, :] = lax.dot_general(
            hid[lo:hi, :], emb[...], (((1,), (1,)), ((), ())), preferred_element_type=f32
        )

    def over_rows(k, pair):
        return jnp.broadcast_to(jnp.concatenate(pair, 1), (128, 128)).T

    for s, p in ((PLUS, P2), (MINUS, P1), (PLUS, P4), (MINUS, P3), (MINUS, P2), (PLUS, P1), (MINUS, P4), (PLUS, P3)):
        got(s, p)

    for k, (dy, dc) in enumerate(yc_peers):
        arrived(wtb.at[at(c - dc, NC) * NY + at(y - dy, NY)], rw.at[k])
    for k in range(TOKENS // 128):
        ga, gb = group(*RHO[2 * k]), group(*RHO[2 * k + 1])
        wrep[128 * k : 128 * k + 128, :] = over_rows(k, [wtb[g, 0:1, 0:ROWS] for g in (ga, gb)])
        trep[128 * k : 128 * k + 128, :] = over_rows(k, [wtb[g, 1:2, 0:ROWS] for g in (ga, gb)])

    for s, p in (
        (PLUS, R2), (PLUS, L2), (PLUS, ZD), (MINUS, R1), (MINUS, L1), (MINUS, ZU),
        (FAR, P2), (FAR, P1), (FAR, P4), (FAR, P3),
        (MINUS, R2), (MINUS, L2), (MINUS, ZD), (PLUS, ZU), (PLUS, R1), (PLUS, L1),
    ):
        got(s, p)
    for load in load_emb:
        load.wait()

    base = ((((y * NC + c) * NX + x) * NZ + z) * VROWS).astype(f32)

    def exps(i, carry):
        r = pl.ds(pl.multiple_of(i * 32, 32), 32)
        t = jnp.tanh(prob[r, :] * (1.0 / soft_cap))
        e = jnp.exp(soft_cap * t - soft_cap)
        q = 1.0 - t * t
        v = e * q
        prob[r, :] = v
        pm[r, :] = v.astype(bf16)
        want = trep[r, :] - base
        lane = lax.broadcasted_iota(jnp.int32, (32, 128), 1).astype(f32)
        total = jnp.zeros((32, 128), f32)
        found = jnp.zeros((32, 128), f32)
        for k in range(VROWS // 128):
            s = slice(128 * k, 128 * k + 128)
            hit = want == lane + float(128 * k)
            hm[r, s] = jnp.where(hit, 1.0, 0.0).astype(bf16)
            total = total + e[:, s]
            found = found + jnp.where(hit, q[:, s], 0.0)
        sums[r, :] = total
        hits[r, :] = found
        return carry

    logits(0, 192)
    for p in (R2, L2, ZD, R1, L1, ZU):
        got(FAR, p)
    arrived(shard(1, OWN), rd.at[3 * NP])
    from_partner(PLUS, MINUS)
    logits(320, 512)
    lax.fori_loop(0, 6, exps, 0)
    from_partner(FAR)
    logits(192, 320)
    lax.fori_loop(6, TOKENS // 32, exps, 0)

    for k in range(TOKENS // 128):
        r = slice(128 * k, 128 * k + 128)
        total = jnp.sum(sums[r, :].T, axis=0, keepdims=True)
        found = jnp.sum(hits[r, :].T, axis=0, keepdims=True)
        for j in range(2):
            lanes = slice(ROWS * j, ROWS * j + ROWS)
            stat[pl.ds(group(*RHO[2 * k + j]), 1), :] = jnp.concatenate([total[:, lanes], found[:, lanes]], 1)

    for k, (dy, dc) in enumerate(yc_peers):
        start(stat, b1.at[k], rb.at[k], y=at(y + dy, NY), c=at(c + dc, NC))
    blocks = [at(x + d, NX) for d in ORDER]

    def for_partner(m, buf, rbuf, sem):
        for i in range(NX):
            v = jnp.dot(m[HALF:, :], emb[:, cols(blocks[i])], preferred_element_type=f32).astype(bf16)
            buf[i, 0:192] = v[64:256]
            buf[i, 192:256] = v[0:64]
            start(buf.at[i], rbuf.at[i], sem.at[i], c=1 - c)

    for_partner(pm, asend, arecv, rda)
    n1 = len(yc_peers)
    total = stat[...]
    for k in range(n1):
        arrived(b1.at[k], rb.at[k])
        total = total + b1[k]
    stat2[...] = total
    for d in range(1, NX):
        start(stat2, b2.at[d - 1], rb.at[n1 + d - 1], x=at(x + d, NX))
    for i in range(NX):
        own[i] = jnp.dot(pm[:HALF, :], emb[:, cols(blocks[i])], preferred_element_type=f32)
    for_partner(hm, tsend, trecv, rdt)
    for d in range(1, NX):
        arrived(b2.at[d - 1], rb.at[n1 + d - 1])
        total = total + b2[d - 1]
    stat3[...] = total
    n2 = n1 + NX - 1
    for d in (4, 3, 5, 2, 6, 1, 7):
        start(stat3, b3.at[d - 1], rb.at[n2 + d - 1], z=at(z + d, NZ))
    for i in range(NX):
        town[i] = jnp.dot(hm[:HALF, :], emb[:, cols(blocks[i])], preferred_element_type=f32).astype(bf16)
    for i in range(NX):
        arrived(arecv.at[i], rda.at[i])
        own[i] = own[i] + arecv[i].astype(f32)
    for i in range(NX):
        arrived(trecv.at[i], rdt.at[i])
        town[i] = town[i] + trecv[i]
    for d in range(1, NZ):
        arrived(b3.at[d - 1], rb.at[n2 + d - 1])
        total = total + b3[d - 1]
    every = total[:, 0:ROWS]
    rate[...] = jnp.concatenate(
        [(1.0 + 2.0 * z_weight * (soft_cap + jnp.log(every))) / every, total[:, ROWS:]], 1
    )
    for k in range(TOKENS // 128):
        r = slice(128 * k, 128 * k + 128)
        pair = [rate[pl.ds(group(*RHO[2 * k + j]), 1), :] for j in range(2)]
        frep[r, :] = over_rows(k, [v[:, 0:ROWS] for v in pair]) * wrep[r, :]
        grep[r, :] = over_rows(k, [v[:, ROWS:] for v in pair]) * wrep[r, :]

    for i, d in enumerate(ORDER):

        def combine(m, carry, i=i):
            r = pl.ds(pl.multiple_of(m * 32, 32), 32)
            f, g = frep[r, :], grep[r, :]
            for k in range(BLK // 128):
                s = slice(128 * k, 128 * k + 128)
                own[i, r, s] = f * own[i, r, s] - g * town[i, r, s].astype(f32)
            return carry

        lax.fori_loop(0, HALF // 32, combine, 0)
        fy[0, i] = own[i, 192:208, :].astype(bf16)
        fy[1, i] = own[i, 208:224, :].astype(bf16)
        start(fy.at[0, i], fyr.at[0, i], rfy.at[i], y=up)
        start(fy.at[1, i], fyr.at[1, i], rfy.at[NX + i], y=down)
        if d == 2:
            for s in range(NY):
                fx[0, s] = own[i, 64 * s + 32 : 64 * s + 48, :].astype(bf16)
                fx[1, s] = own[i, 64 * s + 48 : 64 * s + 64, :].astype(bf16)
            start(fx.at[0], fxr.at[0], rfx.at[0], x=right)
            start(fx.at[1], fxr.at[1], rfx.at[1], x=left)

    def scores(i, carry):
        r = pl.ds(pl.multiple_of(i * 32, 32), 32)
        f, g = frep[r, :], grep[r, :]
        for k in range(VROWS // 128):
            s = slice(128 * k, 128 * k + 128)
            sc[r, s] = f * prob[r, s] - g * hm[r, s].astype(f32)
        return carry

    lax.fori_loop(0, TOKENS // 32, scores, 0)

    for side, (b, dev) in enumerate(((1, right), (2, left))):
        arrived(fxr.at[side], rfx.at[side])
        for s in range(NY):
            lo = 64 * s + 32
            a1, a2 = own[b, lo : lo + 16, :], own[b, lo + 16 : lo + 32, :]
            more = fxr[side, s].astype(f32)
            nx[side, s, 0:16] = (a1 + more if side == 0 else a1).astype(bf16)
            nx[side, s, 16:32] = (a2 + more if side == 1 else a2).astype(bf16)
        start(nx.at[side], nxr.at[side], rnx.at[side], x=dev)
    for i in range(NX):
        for side, (lo, dev) in enumerate(((64, up), (128, down))):
            arrived(fyr.at[side, i], rfy.at[side * NX + i])
            a1, a2 = own[i, lo : lo + 16, :], own[i, lo + 16 : lo + 32, :]
            more = fyr[side, i].astype(f32)
            ny[side, i, 0:16] = (a1 + more if side == 0 else a1).astype(bf16)
            ny[side, i, 16:32] = (a2 + more if side == 1 else a2).astype(bf16)
            start(ny.at[side, i], nyr.at[side, i], rny.at[side * NX + i], y=dev)

    for k in range(VROWS // 128):
        s = slice(128 * k, 128 * k + 128)
        sct[s, :] = sc[:, s].T.astype(bf16)

    def table(i):
        tg_out[:, i * BLK : (i + 1) * BLK] = jnp.dot(
            sct[...], hid[:, i * BLK : (i + 1) * BLK], preferred_element_type=f32
        ).astype(bf16)

    table(0)
    table(1)

    for i, d in enumerate(ORDER):
        total = own[i, 0:32, :]
        for side in range(2):
            arrived(nyr.at[side, i], rny.at[side * NX + i])
            total = total + nyr[side, i].astype(f32)
        if d:
            ys[d - 1] = total.astype(bf16)
            start(ys.at[d - 1], sy.at[d - 1], rty.at[d - 1], x=blocks[i])
        else:
            keep0 = total
    for side in range(2):
        arrived(nxr.at[side], rnx.at[side])

    def x_sum(s):
        return own[NX - 1, 64 * s + 32 : 64 * s + 64, :] + nxr[0, s].astype(f32) + nxr[1, s].astype(f32)

    for s, dy in ((FAR, 2), (PLUS, 1), (MINUS, 3)):
        xs2[dy - 1] = x_sum(s).astype(bf16)
        start(xs2.at[dy - 1], sx.at[dy - 1], rtx.at[dy - 1], y=where[s])
    half = NZ // 2
    zf[0:half] = keep0.reshape(half, ZR, BLK)
    zf[half:NZ] = x_sum(OWN).reshape(half, ZR, BLK)
    table(2)
    keep0 = zf[0:half]
    for d in range(1, NX):
        arrived(sy.at[d - 1], rty.at[d - 1])
        keep0 = keep0 + sy[d - 1].astype(f32).reshape(half, ZR, BLK)
    keep1 = zf[half:NZ]
    for d in range(1, NY):
        arrived(sx.at[d - 1], rtx.at[d - 1])
        keep1 = keep1 + sx[d - 1].astype(f32).reshape(half, ZR, BLK)

    zf[0:half] = keep0
    zf[half:NZ] = keep1
    zs[...] = zf[...].astype(bf16)
    for d in (4, 3, 5, 2, 6, 1, 7):
        zz = at(z + d, NZ)
        start(zs.at[zz], rz.at[d - 1], rzs.at[d - 1], z=zz)
    table(3)
    total = zf[z]
    for d in (1, 7, 2, 6, 3, 5, 4):
        arrived(rz.at[d - 1], rzs.at[d - 1])
        total = total + rz[d - 1].astype(f32)
    gz[z] = total.astype(bf16)
    for d in (4, 3, 5, 2, 6, 1, 7):
        start(gz.at[z], gz.at[z], rzg.at[d - 1], z=at(z + d, NZ))

    def on_to_x(d, zz):
        for dx in (2, 1, 3):
            start(gz.at[zz], gx.at[dx - 1, zz], rxg.at[(dx - 1) * NZ + d], x=at(x + dx, NX))

    on_to_x(0, z)
    for d in (1, 7, 2, 6, 3, 5, 4):
        arrived(gz.at[at(z - d, NZ)], rzg.at[d - 1])
        on_to_x(d, at(z - d, NZ))
    hg_out[:, cols(x)] = gz[...].reshape(ROWS, BLK)
    for dx in range(1, NX):
        for d in range(NZ):
            arrived(gx.at[dx - 1, at(z - d, NZ)], rxg.at[(dx - 1) * NZ + d])
        hg_out[:, cols(at(x - dx, NX))] = gx[dx - 1].reshape(ROWS, BLK)

    for copy in sends:
        copy.wait_send()


def body(hidden, embedding, targets, loss_weight):
    vm = pltpu.VMEM
    dma = pltpu.SemaphoreType.DMA
    inputs = (hidden, embedding, loss_weight.reshape(1, ROWS), targets.reshape(1, ROWS))
    return pl.pallas_call(
        kernel,
        out_shape=(
            jax.ShapeDtypeStruct((ROWS, D), bf16),
            jax.ShapeDtypeStruct((VROWS, D), bf16),
        ),
        in_specs=[pl.BlockSpec(memory_space=pl.ANY)] * 4,
        out_specs=(pl.BlockSpec(memory_space=pltpu.VMEM), pl.BlockSpec(memory_space=pltpu.VMEM)),
        scratch_shapes=[
            vm((1, ROWS), bf16),
            vm((1, ROWS), jnp.int32),
            vm((TOKENS, D), bf16),
            vm((VROWS, D), bf16),
            vm((NC * NY, 2, 128), f32),
            vm((TOKENS, 128), f32),
            vm((TOKENS, 128), f32),
            vm((TOKENS, VROWS), f32),
            vm((TOKENS, 128), f32),
            vm((TOKENS, 128), f32),
            vm((NC * NY, 128), f32),
            vm((NC * NY, 128), f32),
            vm((NC * NY, 128), f32),
            vm((NC * NY, 128), f32),
            vm((TOKENS, 128), f32),
            vm((TOKENS, 128), f32),
            vm((NY * NC - 1, NC * NY, 128), f32),
            vm((NX - 1, NC * NY, 128), f32),
            vm((NZ - 1, NC * NY, 128), f32),
            vm((TOKENS, VROWS), bf16),
            vm((TOKENS, VROWS), bf16),
            vm((TOKENS, VROWS), f32),
            vm((VROWS, TOKENS), bf16),
            vm((NX, HALF, BLK), f32),
            vm((NX, HALF, BLK), bf16),
            vm((NX, HALF, BLK), bf16),
            vm((NX, HALF, BLK), bf16),
            vm((NX, HALF, BLK), bf16),
            vm((NX, HALF, BLK), bf16),
            vm((2, NX, SUB // 2, BLK), bf16),
            vm((2, NX, SUB // 2, BLK), bf16),
            vm((2, NX, SUB, BLK), bf16),
            vm((2, NX, SUB, BLK), bf16),
            vm((2, NY, SUB // 2, BLK), bf16),
            vm((2, NY, SUB // 2, BLK), bf16),
            vm((2, NY, SUB, BLK), bf16),
            vm((2, NY, SUB, BLK), bf16),
            vm((NX - 1, SUB, BLK), bf16),
            vm((NY - 1, SUB, BLK), bf16),
            vm((NX - 1, SUB, BLK), bf16),
            vm((NY - 1, SUB, BLK), bf16),
            vm((NZ, ZR, BLK), f32),
            vm((NZ, ZR, BLK), bf16),
            vm((NZ - 1, ZR, BLK), bf16),
            vm((NZ, ZR, BLK), bf16),
            vm((NX - 1, NZ, ZR, BLK), bf16),
            dma((NX + 3,)),
            dma((180,)),
            dma((30,)),
            dma((31,)),
            dma((NY * NC - 1,)),
            dma((NY * NC + NX + NZ - 3,)),
            dma((NX,)),
            dma((NX,)),
            dma((2 * NX,)),
            dma((2 * NX,)),
            dma((2,)),
            dma((2,)),
            dma((NX - 1,)),
            dma((NY - 1,)),
            dma((NZ - 1,)),
            dma((NZ - 1,)),
            dma(((NX - 1) * NZ,)),
        ],
        compiler_params=pltpu.CompilerParams(collective_id=0, has_side_effects=True, vmem_limit_bytes=44 * 1024 * 1024),
        name="head_backward",
    )(*(pltpu.with_memory_space_constraint(a, pltpu.HBM) for a in inputs))


def solution(mesh):
    finer = Mesh(mesh.devices.reshape(NY, NC, NX, NZ), ("y", "c", "x", "z"))
    dp = ("y", "c")
    both = ("y", "c", "x", "z")
    return jax.shard_map(
        body,
        mesh=finer,
        in_specs=(P(dp, None), P(both, None), P(dp), P(dp)),
        out_specs=(P(dp, None), P(both, None)),
        check_vma=False,
    )
```

```python
import functools

import jax
import jax.numpy as jnp
from jax import lax
from jax.experimental import pallas as pl
from jax.experimental.pallas import tpu as pltpu
from jax.sharding import Mesh
from jax.sharding import PartitionSpec as P

MESH = pl.DeviceIdType.MESH
f32, bf16 = jnp.float32, jnp.bfloat16

NY, NC, NX, NZ = 4, 2, 4, 8
D, VROWS, ROWS = 3584, 768, 64
TOKENS = ROWS * NY * NC
HALF = ROWS * NY
BLK = D // NX
SUB = ROWS // 2
ZR = ROWS // NZ
ORDER = (2, 1, 3, 0)

soft_cap = 30.0
z_weight = 0.002


class Field:
    pass


BUFS = ("fy", "fyr", "ny", "nyr", "fx", "fxr", "nx", "nxr", "ys", "xs2", "sy", "sx", "zf", "zs", "rz")
SEMS = ("rd2", "rfy", "rny", "rfx", "rnx", "rty", "rtx", "rzs")


def kernel(
    hid_in, emb_in, w_in, t_in, hg_out, tg_out,
    w_own, t_own, hid, emb, wtb, wall, trep, prob, sums, fe, fq, stat, stat2, stat3, rate, frep, hrep, b1, b2, b3,
    pm, hm, sc, sct, own, town, asend, arecv, tsend, trecv, gz, gx,
    local_sem, send_sem, ra, rd, rw, rb, rzg, rxg, *fields,
):
    A, T = Field(), Field()
    n = len(BUFS) + len(SEMS)
    for field, refs in ((A, fields[:n]), (T, fields[n:])):
        for name, ref in zip(BUFS + SEMS, refs):
            setattr(field, name, ref)
    A.own, A.send, A.recv, A.m = own, asend, arecv, pm
    T.own, T.send, T.recv, T.m = town, tsend, trecv, hm
    y, c, x, z = (lax.axis_index(a) for a in ("y", "c", "x", "z"))
    rem = lax.rem

    def at(i, n):
        return rem(i + n, n)

    up, down, far = at(y + 1, NY), at(y - 1, NY), at(y + 2, NY)
    right, left = at(x + 1, NX), at(x - 1, NX)
    above, below = at(z + 1, NZ), at(z - 1, NZ)
    OWN, PLUS, MINUS, FAR = range(4)
    where = {OWN: y, PLUS: up, MINUS: down, FAR: far}
    RHO = ((0, OWN), (0, PLUS), (0, MINUS), (0, FAR), (1, FAR), (1, OWN), (1, PLUS), (1, MINUS))
    row_of = {key: ROWS * k for k, key in enumerate(RHO)}
    me = c * NY + y

    def group(e, s):
        return (1 - c if e else c) * NY + where[s]

    sends = []

    def start(src, dst, rsem, **dev):
        copy = pltpu.make_async_remote_copy(
            src_ref=src, dst_ref=dst, send_sem=send_sem.at[len(sends)], recv_sem=rsem, device_id=dev, device_id_type=MESH
        )
        copy.start()
        sends.append(copy)

    def arrived(dst, rsem):
        pltpu.make_async_remote_copy(
            src_ref=dst, dst_ref=dst, send_sem=send_sem.at[0], recv_sem=rsem, device_id={"c": 1 - c}, device_id_type=MESH
        ).wait_recv()

    def cols(q):
        return pl.ds(pl.multiple_of(q * BLK, 128), BLK)

    def shard(e, s):
        return hid.at[row_of[e, s] : row_of[e, s] + ROWS]

    def piece(e, s, q, lo, hi):
        return hid.at[row_of[e, s] : row_of[e, s] + ROWS, pl.ds(pl.multiple_of(q * BLK + lo, 128), hi - lo)]

    load_own = [
        pltpu.make_async_copy(hid_in, shard(0, OWN), local_sem.at[NX]),
        pltpu.make_async_copy(w_in, w_own, local_sem.at[NX + 1]),
        pltpu.make_async_copy(t_in, t_own, local_sem.at[NX + 2]),
    ]
    load_emb = []
    for k in range(NX):
        part = pl.ds(k * (VROWS // NX), VROWS // NX)
        load_emb.append(pltpu.make_async_copy(emb_in.at[part], emb.at[part], local_sem.at[k]))
    for load in load_own + load_emb:
        load.start()

    barrier = pltpu.get_barrier_semaphore()
    yc_peers = [(dy, dc) for dy in range(NY) for dc in range(NC) if (dy, dc) != (0, 0)]
    for dy, dc in yc_peers:
        pl.semaphore_signal(barrier, inc=1, device_id={"y": at(y + dy, NY), "c": at(c + dc, NC)}, device_id_type=MESH)
    for d in range(1, NX):
        pl.semaphore_signal(barrier, inc=1, device_id={"x": at(x + d, NX)}, device_id_type=MESH)
    for d in range(1, NZ):
        pl.semaphore_signal(barrier, inc=1, device_id={"z": at(z + d, NZ)}, device_id_type=MESH)

    for load in load_own:
        load.wait()
    none = jnp.zeros((1, ROWS), f32)
    wtb[me] = jnp.concatenate(
        [jnp.concatenate([v, none], 1) for v in (w_own[...].astype(f32), t_own[...].astype(f32))], 0
    )

    pl.semaphore_wait(barrier, len(yc_peers) + NX - 1 + NZ - 1)

    k0 = rem(x + 2 * z, NX)
    kp, km, k2 = rem(k0 + 1, NX), rem(k0 + 3, NX), rem(k0 + 2, NX)
    P1, P2, P3, P4, R1, R2, L1, L2, ZU, ZD = range(10)
    parts = (
        (k0, 0, 512), (k0, 512, BLK), (kp, 0, 256), (km, 0, 256),
        (kp, 256, 512), (kp, 512, BLK), (km, 256, 512), (km, 512, BLK),
        (k2, 0, 512), (k2, 512, BLK),
    )
    NP = len(parts)

    def slot(s, p):
        return (s - 1) * NP + p

    def to_up(s, p):
        start(piece(0, s, *parts[p]), piece(0, MINUS if s == OWN else FAR, *parts[p]), ra.at[slot(MINUS if s == OWN else FAR, p)], y=up)

    def to_down(s, p):
        start(piece(0, s, *parts[p]), piece(0, PLUS if s == OWN else FAR, *parts[p]), ra.at[slot(PLUS if s == OWN else FAR, p)], y=down)

    for k, (dy, dc) in enumerate(yc_peers):
        start(wtb.at[me], wtb.at[me], rw.at[k], y=at(y + dy, NY), c=at(c + dc, NC))
    for p, q in ((P1, P2), (P3, P4), (P2, P1), (P4, P3)):
        to_up(OWN, p)
        to_down(OWN, q)
    start(shard(0, OWN), shard(1, OWN), rd.at[3 * NP], c=1 - c)

    def got(s, p):
        part = piece(0, s, *parts[p])
        arrived(part, ra.at[slot(s, p)])
        if s == MINUS and p in (P1, P3):
            to_up(s, p)
        if s == PLUS and p in (P2, P4):
            to_down(s, p)
        if p in (P1, P2):
            sub = piece(0, s, k0, 256, 512) if p == P1 else part
            start(sub, sub, ra.at[slot(s, R1 if p == P1 else R2)], x=left)
            start(sub, sub, ra.at[slot(s, L1 if p == P1 else L2)], x=right)
            if p == P1:
                start(part, part, ra.at[slot(s, ZU)], z=below)
            else:
                start(part, part, ra.at[slot(s, ZD)], z=above)
        start(part, piece(1, s, *parts[p]), rd.at[slot(s, p)], c=1 - c)

    def from_partner(*ss):
        for s in ss:
            for p in range(NP):
                arrived(piece(1, s, *parts[p]), rd.at[slot(s, p)])

    def logits(lo, hi):
        prob[lo:hi, :] = lax.dot_general(
            hid[lo:hi, :], emb[...], (((1,), (1,)), ((), ())), preferred_element_type=f32
        )

    def over_rows(pair):
        return jnp.broadcast_to(jnp.concatenate(pair, 1), (128, 128)).T

    for s, p in ((PLUS, P2), (MINUS, P1)):
        got(s, p)

    for load in load_emb:
        load.wait()
    for k, (dy, dc) in enumerate(yc_peers):
        arrived(wtb.at[at(c - dc, NC) * NY + at(y - dy, NY)], rw.at[k])
    for k in range(TOKENS // 128):
        trep[128 * k : 128 * k + 128, :] = over_rows([wtb[group(*RHO[2 * k + j]), 1:2, 0:ROWS] for j in range(2)])
    for g in range(NC * NY):
        wall[g : g + 1, :] = wtb[g, 0:1, :]

    base = ((((y * NC + c) * NX + x) * NZ + z) * VROWS).astype(f32)

    def onehots(i, carry):
        r = pl.ds(pl.multiple_of(i * 32, 32), 32)
        want = trep[r, :] - base
        lane = lax.broadcasted_iota(jnp.int32, (32, 128), 1).astype(f32)
        for k in range(VROWS // 128):
            s = slice(128 * k, 128 * k + 128)
            hm[r, s] = jnp.where(want == lane + float(128 * k), 1.0, 0.0).astype(bf16)
        return carry

    lax.fori_loop(0, TOKENS // 32, onehots, 0)

    blocks = [at(x + d, NX) for d in ORDER]

    def for_partner(F, i):
        v = jnp.dot(F.m[HALF:, :], emb[:, cols(blocks[i])], preferred_element_type=f32).astype(bf16)
        F.send[i, 0:192] = v[64:256]
        F.send[i, 192:256] = v[0:64]
        start(F.send.at[i], F.recv.at[i], F.rd2.at[i], c=1 - c)

    def for_self(F, i):
        F.own[i] = jnp.dot(F.m[:HALF, :], emb[:, cols(blocks[i])], preferred_element_type=f32).astype(F.own.dtype)

    def of_chip(F, i):
        arrived(F.recv.at[i], F.rd2.at[i])
        F.own[i] = F.own[i] + F.recv[i].astype(F.own.dtype)

    def far_halves(F, i):
        F.fy[0, i] = F.own[i, 192:208, :].astype(bf16)
        F.fy[1, i] = F.own[i, 208:224, :].astype(bf16)
        start(F.fy.at[0, i], F.fyr.at[0, i], F.rfy.at[i], y=up)
        start(F.fy.at[1, i], F.fyr.at[1, i], F.rfy.at[NX + i], y=down)
        if ORDER[i] == 2:
            for s in range(NY):
                F.fx[0, s] = F.own[i, 64 * s + 32 : 64 * s + 48, :].astype(bf16)
                F.fx[1, s] = F.own[i, 64 * s + 48 : 64 * s + 64, :].astype(bf16)
            start(F.fx.at[0], F.fxr.at[0], F.rfx.at[0], x=right)
            start(F.fx.at[1], F.fxr.at[1], F.rfx.at[1], x=left)

    def with_far(F, i, lo, side, more):
        a1 = F.own[i, lo : lo + 16, :].astype(f32)
        a2 = F.own[i, lo + 16 : lo + 32, :].astype(f32)
        more = more.astype(f32)
        return (a1 + more if side == 0 else a1).astype(bf16), (a2 + more if side == 1 else a2).astype(bf16)

    def near_x(F):
        for side, (b, dev) in enumerate(((1, right), (2, left))):
            arrived(F.fxr.at[side], F.rfx.at[side])
            for s in range(NY):
                F.nx[side, s, 0:16], F.nx[side, s, 16:32] = with_far(F, b, 64 * s + 32, side, F.fxr[side, s])
            start(F.nx.at[side], F.nxr.at[side], F.rnx.at[side], x=dev)

    def near_y(F, i):
        for side, (lo, dev) in enumerate(((64, up), (128, down))):
            arrived(F.fyr.at[side, i], F.rfy.at[side * NX + i])
            F.ny[side, i, 0:16], F.ny[side, i, 16:32] = with_far(F, i, lo, side, F.fyr[side, i])
            start(F.ny.at[side, i], F.nyr.at[side, i], F.rny.at[side * NX + i], y=dev)

    half = NZ // 2

    def stage_two(F):
        for i, d in enumerate(ORDER):
            total = F.own[i, 0:32, :].astype(f32)
            for side in range(2):
                arrived(F.nyr.at[side, i], F.rny.at[side * NX + i])
                total = total + F.nyr[side, i].astype(f32)
            if d:
                F.ys[d - 1] = total.astype(bf16)
                start(F.ys.at[d - 1], F.sy.at[d - 1], F.rty.at[d - 1], x=blocks[i])
            else:
                F.zf[0:half] = total.reshape(half, ZR, BLK)
        for side in range(2):
            arrived(F.nxr.at[side], F.rnx.at[side])
        for s, dy in ((FAR, 2), (PLUS, 1), (MINUS, 3), (OWN, 0)):
            total = F.own[NX - 1, 64 * s_row[s] + 32 : 64 * s_row[s] + 64, :].astype(f32)
            total = total + F.nxr[0, s_row[s]].astype(f32) + F.nxr[1, s_row[s]].astype(f32)
            if dy:
                F.xs2[dy - 1] = total.astype(bf16)
                start(F.xs2.at[dy - 1], F.sx.at[dy - 1], F.rtx.at[dy - 1], y=where[s])
            else:
                F.zf[half:NZ] = total.reshape(half, ZR, BLK)

    s_row = {s: row_of[0, s] // ROWS for s in range(4)}

    def to_z(F):
        total = F.zf[0:half]
        for d in range(1, NX):
            arrived(F.sy.at[d - 1], F.rty.at[d - 1])
            total = total + F.sy[d - 1].astype(f32).reshape(half, ZR, BLK)
        F.zf[0:half] = total
        F.zs[0:half] = total.astype(bf16)
        total = F.zf[half:NZ]
        for d in range(1, NY):
            arrived(F.sx.at[d - 1], F.rtx.at[d - 1])
            total = total + F.sx[d - 1].astype(f32).reshape(half, ZR, BLK)
        F.zf[half:NZ] = total
        F.zs[half:NZ] = total.astype(bf16)
        for d in (4, 3, 5, 2, 6, 1, 7):
            zz = at(z + d, NZ)
            start(F.zs.at[zz], F.rz.at[d - 1], F.rzs.at[d - 1], z=zz)

    def z_sum(F):
        total = F.zf[z]
        for d in (1, 7, 2, 6, 3, 5, 4):
            arrived(F.rz.at[d - 1], F.rzs.at[d - 1])
            total = total + F.rz[d - 1].astype(f32)
        return total

    def exps(i, carry):
        r = pl.ds(pl.multiple_of(i * 32, 32), 32)
        t = jnp.tanh(prob[r, :] * (1.0 / soft_cap))
        e = jnp.exp(soft_cap * t - soft_cap)
        q = 1.0 - t * t
        total = jnp.zeros((32, 128), f32)
        found_e = jnp.zeros((32, 128), f32)
        found_q = jnp.zeros((32, 128), f32)
        for k in range(VROWS // 128):
            s = slice(128 * k, 128 * k + 128)
            hit = hm[r, s].astype(f32) > 0.5
            v = jnp.where(hit, 0.0, e[:, s] * q[:, s])
            prob[r, s] = v
            pm[r, s] = v.astype(bf16)
            total = total + e[:, s]
            found_e = found_e + jnp.where(hit, e[:, s], 0.0)
            found_q = found_q + jnp.where(hit, q[:, s], 0.0)
        sums[r, :] = total
        fe[r, :] = found_e
        fq[r, :] = found_q
        return carry

    for k, step in enumerate((
        ((PLUS, P4), (MINUS, P3)), ((MINUS, P2), (PLUS, P1)), ((MINUS, P4), (PLUS, P3)),
        ((PLUS, R2), (PLUS, L2), (PLUS, ZD)), ((MINUS, R1), (MINUS, L1), (MINUS, ZU), (FAR, P2)),
        ((FAR, P1), (FAR, P4)), ((FAR, P3), (MINUS, R2), (MINUS, L2), (MINUS, ZD)), ((PLUS, ZU), (PLUS, R1), (PLUS, L1)),
    )):
        for s, p in step:
            got(s, p)
        if k < NX:
            for_partner(T, k)
        else:
            for_self(T, k - NX)
            of_chip(T, k - NX)
            far_halves(T, k - NX)
    logits(0, 192)
    for p in (R2, L2, ZD, R1, L1, ZU):
        got(FAR, p)
    arrived(shard(1, OWN), rd.at[3 * NP])
    from_partner(PLUS, MINUS)
    logits(320, 512)
    near_x(T)
    for i in range(NX):
        near_y(T, i)
    from_partner(FAR)
    logits(192, 320)
    lax.fori_loop(0, TOKENS // 32, exps, 0)

    def stats():
        for k in range(TOKENS // 128):
            r = slice(128 * k, 128 * k + 128)
            three = [jnp.sum(v[r, :].T, axis=0, keepdims=True) for v in (sums, fe, fq)]
            for j in range(2):
                lanes = slice(ROWS * j, ROWS * j + ROWS)
                stat[pl.ds(group(*RHO[2 * k + j]), 1), :] = jnp.concatenate([v[:, lanes] for v in three] + [none], 1)
        for k, (dy, dc) in enumerate(yc_peers):
            start(stat, b1.at[k], rb.at[k], y=at(y + dy, NY), c=at(c + dc, NC))

    n1 = len(yc_peers)
    n2 = n1 + NX - 1
    for_partner(A, 0)
    stats()
    for_partner(A, 1)
    for_self(A, 0)
    of_chip(A, 0)
    far_halves(A, 0)
    for_partner(A, 2)
    for_self(A, 1)
    of_chip(A, 1)
    far_halves(A, 1)
    total = stat[...]
    for k in range(n1):
        arrived(b1.at[k], rb.at[k])
        total = total + b1[k]
    stat2[...] = total
    for d in range(1, NX):
        start(stat2, b2.at[d - 1], rb.at[n1 + d - 1], x=at(x + d, NX))
    for_partner(A, 3)
    for_self(A, 2)
    of_chip(A, 2)
    far_halves(A, 2)
    stage_two(T)
    for_self(A, 3)
    of_chip(A, 3)
    far_halves(A, 3)
    total = stat2[...]
    for d in range(1, NX):
        arrived(b2.at[d - 1], rb.at[n1 + d - 1])
        total = total + b2[d - 1]
    stat3[...] = total
    for d in (4, 3, 5, 2, 6, 1, 7):
        start(stat3, b3.at[d - 1], rb.at[n2 + d - 1], z=at(z + d, NZ))
    near_x(A)
    for i in range(NX):
        near_y(A, i)
    to_z(T)

    total = stat3[...]
    for d in range(1, NZ):
        arrived(b3.at[d - 1], rb.at[n2 + d - 1])
        total = total + b3[d - 1]
    every, e_hit, q_hit = (total[:, ROWS * k : ROWS * k + ROWS] for k in range(3))
    w = wall[:, 0:ROWS]
    factor = w * (1.0 + 2.0 * z_weight * (soft_cap + jnp.log(every))) / every
    rate[...] = jnp.concatenate([factor, (factor * e_hit - w) * q_hit], 1)
    for k in range(TOKENS // 128):
        r = slice(128 * k, 128 * k + 128)
        pair = [rate[pl.ds(group(*RHO[2 * k + j]), 1), :] for j in range(2)]
        frep[r, :] = over_rows([v[:, 0:ROWS] for v in pair])
        hrep[r, :] = over_rows([v[:, ROWS:] for v in pair])

    def scores(i, carry):
        r = pl.ds(pl.multiple_of(i * 32, 32), 32)
        f, h = frep[r, :], hrep[r, :]
        for k in range(VROWS // 128):
            s = slice(128 * k, 128 * k + 128)
            sc[r, s] = f * prob[r, s] + h * hm[r, s].astype(f32)
        return carry

    def table(i):
        tg_out[:, i * BLK : (i + 1) * BLK] = jnp.dot(
            sct[...], hid[:, i * BLK : (i + 1) * BLK], preferred_element_type=f32
        ).astype(bf16)

    lax.fori_loop(0, TOKENS // 32, scores, 0)
    for k in range(VROWS // 128):
        s = slice(128 * k, 128 * k + 128)
        sct[s, :] = sc[:, s].T.astype(bf16)
    table(0)
    table(1)
    stage_two(A)
    table(2)
    table(3)
    to_z(A)
    mine = pl.ds(pl.multiple_of(z * ZR, ZR), ZR)
    t_part = z_sum(T)
    a_part = z_sum(A)
    f, h = frep[mine, :], hrep[mine, :]
    for k in range(BLK // 128):
        s = slice(128 * k, 128 * k + 128)
        gz[z, :, s] = (f * a_part[:, s] + h * t_part[:, s]).astype(bf16)
    for d in (4, 3, 5, 2, 6, 1, 7):
        start(gz.at[z], gz.at[z], rzg.at[d - 1], z=at(z + d, NZ))

    def on_to_x(d, zz):
        for dx in (2, 1, 3):
            start(gz.at[zz], gx.at[dx - 1, zz], rxg.at[(dx - 1) * NZ + d], x=at(x + dx, NX))

    on_to_x(0, z)
    for d in (1, 7, 2, 6, 3, 5, 4):
        arrived(gz.at[at(z - d, NZ)], rzg.at[d - 1])
        on_to_x(d, at(z - d, NZ))
    hg_out[:, cols(x)] = gz[...].reshape(ROWS, BLK)
    for dx in range(1, NX):
        for d in range(NZ):
            arrived(gx.at[dx - 1, at(z - d, NZ)], rxg.at[(dx - 1) * NZ + d])
        hg_out[:, cols(at(x - dx, NX))] = gx[dx - 1].reshape(ROWS, BLK)

    for copy in sends:
        copy.wait_send()


def body(hidden, embedding, targets, loss_weight):
    vm = pltpu.VMEM
    dma = pltpu.SemaphoreType.DMA
    inputs = (hidden, embedding, loss_weight.reshape(1, ROWS), targets.reshape(1, ROWS))
    return pl.pallas_call(
        kernel,
        out_shape=(
            jax.ShapeDtypeStruct((ROWS, D), bf16),
            jax.ShapeDtypeStruct((VROWS, D), bf16),
        ),
        in_specs=[pl.BlockSpec(memory_space=pl.ANY)] * 4,
        out_specs=(pl.BlockSpec(memory_space=pltpu.VMEM), pl.BlockSpec(memory_space=pltpu.VMEM)),
        scratch_shapes=[
            vm((1, ROWS), bf16),
            vm((1, ROWS), jnp.int32),
            vm((TOKENS, D), bf16),
            vm((VROWS, D), bf16),
            vm((NC * NY, 2, 128), f32),
            vm((NC * NY, 128), f32),
            vm((TOKENS, 128), f32),
            vm((TOKENS, VROWS), f32),
            vm((TOKENS, 128), f32),
            vm((TOKENS, 128), f32),
            vm((TOKENS, 128), f32),
            vm((NC * NY, 256), f32),
            vm((NC * NY, 256), f32),
            vm((NC * NY, 256), f32),
            vm((NC * NY, 128), f32),
            vm((TOKENS, 128), f32),
            vm((TOKENS, 128), f32),
            vm((NY * NC - 1, NC * NY, 256), f32),
            vm((NX - 1, NC * NY, 256), f32),
            vm((NZ - 1, NC * NY, 256), f32),
            vm((TOKENS, VROWS), bf16),
            vm((TOKENS, VROWS), bf16),
            vm((TOKENS, VROWS), f32),
            vm((VROWS, TOKENS), bf16),
            vm((NX, HALF, BLK), f32),
            vm((NX, HALF, BLK), bf16),
            vm((NX, HALF, BLK), bf16),
            vm((NX, HALF, BLK), bf16),
            vm((NX, HALF, BLK), bf16),
            vm((NX, HALF, BLK), bf16),
            vm((NZ, ZR, BLK), bf16),
            vm((NX - 1, NZ, ZR, BLK), bf16),
            dma((NX + 3,)),
            dma((230,)),
            dma((30,)),
            dma((31,)),
            dma((NY * NC - 1,)),
            dma((NY * NC + NX + NZ - 3,)),
            dma((NZ - 1,)),
            dma(((NX - 1) * NZ,)),
        ]
        + 2
        * [
            vm((2, NX, SUB // 2, BLK), bf16),
            vm((2, NX, SUB // 2, BLK), bf16),
            vm((2, NX, SUB, BLK), bf16),
            vm((2, NX, SUB, BLK), bf16),
            vm((2, NY, SUB // 2, BLK), bf16),
            vm((2, NY, SUB // 2, BLK), bf16),
            vm((2, NY, SUB, BLK), bf16),
            vm((2, NY, SUB, BLK), bf16),
            vm((NX - 1, SUB, BLK), bf16),
            vm((NY - 1, SUB, BLK), bf16),
            vm((NX - 1, SUB, BLK), bf16),
            vm((NY - 1, SUB, BLK), bf16),
            vm((NZ, ZR, BLK), f32),
            vm((NZ, ZR, BLK), bf16),
            vm((NZ - 1, ZR, BLK), bf16),
            dma((NX,)),
            dma((2 * NX,)),
            dma((2 * NX,)),
            dma((2,)),
            dma((2,)),
            dma((NX - 1,)),
            dma((NY - 1,)),
            dma((NZ - 1,)),
        ],
        compiler_params=pltpu.CompilerParams(collective_id=0, has_side_effects=True, vmem_limit_bytes=44 * 1024 * 1024),
        name="head_backward",
    )(*(pltpu.with_memory_space_constraint(a, pltpu.HBM) for a in inputs))


def solution(mesh):
    finer = Mesh(mesh.devices.reshape(NY, NC, NX, NZ), ("y", "c", "x", "z"))
    dp = ("y", "c")
    both = ("y", "c", "x", "z")
    return jax.shard_map(
        body,
        mesh=finer,
        in_specs=(P(dp, None), P(both, None), P(dp), P(dp)),
        out_specs=(P(dp, None), P(both, None)),
        check_vma=False,
    )
```

```python
import functools

import jax
import jax.numpy as jnp
from jax import lax
from jax.experimental import pallas as pl
from jax.experimental.pallas import tpu as pltpu
from jax.sharding import Mesh
from jax.sharding import PartitionSpec as P

MESH = pl.DeviceIdType.MESH
f32, bf16 = jnp.float32, jnp.bfloat16

NY, NC, NX, NZ = 4, 2, 4, 8
D, VROWS, ROWS = 3584, 768, 64
TOKENS = ROWS * NY * NC
HALF = ROWS * NY
BLK = D // NX
SUB = ROWS // 2
ZR = ROWS // NZ
ORDER = (2, 1, 3, 0)

soft_cap = 30.0
z_weight = 0.002


class Field:
    pass


BUFS = ("fy", "fyr", "ny", "nyr", "fx", "fxr", "nx", "nxr", "ys", "xs2", "sy", "sx", "zf", "zs", "rz")
SEMS = ("rd2", "rfy", "rny", "rfx", "rnx", "rty", "rtx", "rzs")


def kernel(
    hid_in, emb_in, w_in, t_in, hg_out, tg_out,
    w_own, t_own, hid, emb, wtb, wall, trep, prob, sums, fe, fq, stat, stat2, stat3, rate, frep, hrep, b1, b2, b3,
    pm, hm, sc, sct, own, town, asend, arecv, tsend, trecv, gz, gx,
    local_sem, send_sem, ra, rd, rw, rb, rzg, rxg, *fields,
):
    A, T = Field(), Field()
    n = len(BUFS) + len(SEMS)
    for field, refs in ((A, fields[:n]), (T, fields[n:])):
        for name, ref in zip(BUFS + SEMS, refs):
            setattr(field, name, ref)
    A.own, A.send, A.recv, A.m = own, asend, arecv, pm
    T.own, T.send, T.recv, T.m = town, tsend, trecv, hm
    y, c, x, z = (lax.axis_index(a) for a in ("y", "c", "x", "z"))
    rem = lax.rem

    def at(i, n):
        return rem(i + n, n)

    up, down, far = at(y + 1, NY), at(y - 1, NY), at(y + 2, NY)
    right, left = at(x + 1, NX), at(x - 1, NX)
    above, below = at(z + 1, NZ), at(z - 1, NZ)
    OWN, PLUS, MINUS, FAR = range(4)
    where = {OWN: y, PLUS: up, MINUS: down, FAR: far}
    RHO = ((0, OWN), (0, PLUS), (0, MINUS), (0, FAR), (1, FAR), (1, OWN), (1, PLUS), (1, MINUS))
    row_of = {key: ROWS * k for k, key in enumerate(RHO)}
    me = c * NY + y

    def group(e, s):
        return (1 - c if e else c) * NY + where[s]

    sends = []

    def start(src, dst, rsem, **dev):
        copy = pltpu.make_async_remote_copy(
            src_ref=src, dst_ref=dst, send_sem=send_sem.at[len(sends)], recv_sem=rsem, device_id=dev, device_id_type=MESH
        )
        copy.start()
        sends.append(copy)

    drained = []

    def drain(until):
        for copy in sends[len(drained) : until]:
            copy.wait_send()
            drained.append(copy)

    def arrived(dst, rsem):
        pltpu.make_async_remote_copy(
            src_ref=dst, dst_ref=dst, send_sem=send_sem.at[0], recv_sem=rsem, device_id={"c": 1 - c}, device_id_type=MESH
        ).wait_recv()

    def cols(q):
        return pl.ds(pl.multiple_of(q * BLK, 128), BLK)

    def shard(e, s):
        return hid.at[row_of[e, s] : row_of[e, s] + ROWS]

    def piece(e, s, q, lo, hi):
        return hid.at[row_of[e, s] : row_of[e, s] + ROWS, pl.ds(pl.multiple_of(q * BLK + lo, 128), hi - lo)]

    load_own = [
        pltpu.make_async_copy(hid_in, shard(0, OWN), local_sem.at[NX]),
        pltpu.make_async_copy(w_in, w_own, local_sem.at[NX + 1]),
        pltpu.make_async_copy(t_in, t_own, local_sem.at[NX + 2]),
    ]
    load_emb = []
    for k in range(NX):
        part = pl.ds(k * (VROWS // NX), VROWS // NX)
        load_emb.append(pltpu.make_async_copy(emb_in.at[part], emb.at[part], local_sem.at[k]))
    for load in load_own + load_emb:
        load.start()

    barrier = pltpu.get_barrier_semaphore()
    yc_peers = [(dy, dc) for dy in range(NY) for dc in range(NC) if (dy, dc) != (0, 0)]
    for dy, dc in yc_peers:
        pl.semaphore_signal(barrier, inc=1, device_id={"y": at(y + dy, NY), "c": at(c + dc, NC)}, device_id_type=MESH)
    for d in range(1, NX):
        pl.semaphore_signal(barrier, inc=1, device_id={"x": at(x + d, NX)}, device_id_type=MESH)
    for d in range(1, NZ):
        pl.semaphore_signal(barrier, inc=1, device_id={"z": at(z + d, NZ)}, device_id_type=MESH)

    for load in load_own:
        load.wait()
    none = jnp.zeros((1, ROWS), f32)
    wtb[me] = jnp.concatenate(
        [jnp.concatenate([v, none], 1) for v in (w_own[...].astype(f32), t_own[...].astype(f32))], 0
    )

    pl.semaphore_wait(barrier, len(yc_peers) + NX - 1 + NZ - 1)

    k0 = rem(x + 2 * z, NX)
    kp, km, k2 = rem(k0 + 1, NX), rem(k0 + 3, NX), rem(k0 + 2, NX)
    P1, P2, P3, P4, R1, R2, L1, L2, ZU, ZD = range(10)
    parts = (
        (k0, 0, 512), (k0, 512, BLK), (kp, 0, 256), (km, 0, 256),
        (kp, 256, 512), (kp, 512, BLK), (km, 256, 512), (km, 512, BLK),
        (k2, 0, 512), (k2, 512, BLK),
    )
    NP = len(parts)

    def slot(s, p):
        return (s - 1) * NP + p

    def to_up(s, p):
        start(piece(0, s, *parts[p]), piece(0, MINUS if s == OWN else FAR, *parts[p]), ra.at[slot(MINUS if s == OWN else FAR, p)], y=up)

    def to_down(s, p):
        start(piece(0, s, *parts[p]), piece(0, PLUS if s == OWN else FAR, *parts[p]), ra.at[slot(PLUS if s == OWN else FAR, p)], y=down)

    for k, (dy, dc) in enumerate(yc_peers):
        start(wtb.at[me], wtb.at[me], rw.at[k], y=at(y + dy, NY), c=at(c + dc, NC))
    for p, q in ((P1, P2), (P3, P4), (P2, P1), (P4, P3)):
        to_up(OWN, p)
        to_down(OWN, q)
    start(shard(0, OWN), shard(1, OWN), rd.at[3 * NP], c=1 - c)

    def got(s, p):
        part = piece(0, s, *parts[p])
        arrived(part, ra.at[slot(s, p)])
        if s == MINUS and p in (P1, P3):
            to_up(s, p)
        if s == PLUS and p in (P2, P4):
            to_down(s, p)
        if p in (P1, P2):
            sub = piece(0, s, k0, 256, 512) if p == P1 else part
            start(sub, sub, ra.at[slot(s, R1 if p == P1 else R2)], x=left)
            start(sub, sub, ra.at[slot(s, L1 if p == P1 else L2)], x=right)
            if p == P1:
                start(part, part, ra.at[slot(s, ZU)], z=below)
            else:
                start(part, part, ra.at[slot(s, ZD)], z=above)
        start(part, piece(1, s, *parts[p]), rd.at[slot(s, p)], c=1 - c)

    def from_partner(*ps):
        for p in ps:
            for s in (PLUS, MINUS, FAR):
                arrived(piece(1, s, *parts[p]), rd.at[slot(s, p)])

    def logits(q, first_one):
        out = lax.dot_general(
            hid[:, cols(q)], emb[:, cols(q)], (((1,), (1,)), ((), ())), preferred_element_type=f32
        )
        prob[...] = out if first_one else prob[...] + out

    def over_rows(pair):
        return jnp.broadcast_to(jnp.concatenate(pair, 1), (128, 128)).T

    for s, p in ((PLUS, P2), (MINUS, P1)):
        got(s, p)

    for load in load_emb:
        load.wait()
    for k, (dy, dc) in enumerate(yc_peers):
        arrived(wtb.at[at(c - dc, NC) * NY + at(y - dy, NY)], rw.at[k])
    for k in range(TOKENS // 128):
        trep[128 * k : 128 * k + 128, :] = over_rows([wtb[group(*RHO[2 * k + j]), 1:2, 0:ROWS] for j in range(2)])
    for g in range(NC * NY):
        wall[g : g + 1, :] = wtb[g, 0:1, :]

    base = ((((y * NC + c) * NX + x) * NZ + z) * VROWS).astype(f32)

    def onehots(i, carry):
        r = pl.ds(pl.multiple_of(i * 32, 32), 32)
        want = trep[r, :] - base
        lane = lax.broadcasted_iota(jnp.int32, (32, 128), 1).astype(f32)
        for k in range(VROWS // 128):
            s = slice(128 * k, 128 * k + 128)
            hm[r, s] = jnp.where(want == lane + float(128 * k), 1.0, 0.0).astype(bf16)
        return carry

    lax.fori_loop(0, TOKENS // 32, onehots, 0)

    blocks = [at(x + d, NX) for d in ORDER]

    def product(F, i):
        v = jnp.dot(F.m[...], emb[:, cols(blocks[i])], preferred_element_type=f32)
        F.send[i, 0:192] = v[HALF + 64 :].astype(bf16)
        F.send[i, 192:256] = v[HALF : HALF + 64].astype(bf16)
        start(F.send.at[i], F.recv.at[i], F.rd2.at[i], c=1 - c)
        F.own[i] = v[:HALF].astype(F.own.dtype)

    def of_chip(F, i):
        arrived(F.recv.at[i], F.rd2.at[i])
        F.own[i] = F.own[i] + F.recv[i].astype(F.own.dtype)

    def far_halves(F, i):
        F.fy[0, i] = F.own[i, 192:208, :].astype(bf16)
        F.fy[1, i] = F.own[i, 208:224, :].astype(bf16)
        start(F.fy.at[0, i], F.fyr.at[0, i], F.rfy.at[i], y=up)
        start(F.fy.at[1, i], F.fyr.at[1, i], F.rfy.at[NX + i], y=down)
        if ORDER[i] == 2:
            for s in range(NY):
                F.fx[0, s] = F.own[i, 64 * s + 32 : 64 * s + 48, :].astype(bf16)
                F.fx[1, s] = F.own[i, 64 * s + 48 : 64 * s + 64, :].astype(bf16)
            start(F.fx.at[0], F.fxr.at[0], F.rfx.at[0], x=right)
            start(F.fx.at[1], F.fxr.at[1], F.rfx.at[1], x=left)

    def with_far(F, i, lo, side, more):
        a1 = F.own[i, lo : lo + 16, :].astype(f32)
        a2 = F.own[i, lo + 16 : lo + 32, :].astype(f32)
        more = more.astype(f32)
        return (a1 + more if side == 0 else a1).astype(bf16), (a2 + more if side == 1 else a2).astype(bf16)

    def near_x(F):
        for side, (b, dev) in enumerate(((1, right), (2, left))):
            arrived(F.fxr.at[side], F.rfx.at[side])
            for s in range(NY):
                F.nx[side, s, 0:16], F.nx[side, s, 16:32] = with_far(F, b, 64 * s + 32, side, F.fxr[side, s])
            start(F.nx.at[side], F.nxr.at[side], F.rnx.at[side], x=dev)

    def near_y(F, i):
        for side, (lo, dev) in enumerate(((64, up), (128, down))):
            arrived(F.fyr.at[side, i], F.rfy.at[side * NX + i])
            F.ny[side, i, 0:16], F.ny[side, i, 16:32] = with_far(F, i, lo, side, F.fyr[side, i])
            start(F.ny.at[side, i], F.nyr.at[side, i], F.rny.at[side * NX + i], y=dev)

    half = NZ // 2

    def stage_two(F):
        for i, d in enumerate(ORDER):
            total = F.own[i, 0:32, :].astype(f32)
            for side in range(2):
                arrived(F.nyr.at[side, i], F.rny.at[side * NX + i])
                total = total + F.nyr[side, i].astype(f32)
            if d:
                F.ys[d - 1] = total.astype(bf16)
                start(F.ys.at[d - 1], F.sy.at[d - 1], F.rty.at[d - 1], x=blocks[i])
            else:
                F.zf[0:half] = total.reshape(half, ZR, BLK)
        for side in range(2):
            arrived(F.nxr.at[side], F.rnx.at[side])
        for s, dy in ((FAR, 2), (PLUS, 1), (MINUS, 3), (OWN, 0)):
            total = F.own[NX - 1, 64 * s_row[s] + 32 : 64 * s_row[s] + 64, :].astype(f32)
            total = total + F.nxr[0, s_row[s]].astype(f32) + F.nxr[1, s_row[s]].astype(f32)
            if dy:
                F.xs2[dy - 1] = total.astype(bf16)
                start(F.xs2.at[dy - 1], F.sx.at[dy - 1], F.rtx.at[dy - 1], y=where[s])
            else:
                F.zf[half:NZ] = total.reshape(half, ZR, BLK)

    s_row = {s: row_of[0, s] // ROWS for s in range(4)}

    def to_z(F):
        total = F.zf[0:half]
        for d in range(1, NX):
            arrived(F.sy.at[d - 1], F.rty.at[d - 1])
            total = total + F.sy[d - 1].astype(f32).reshape(half, ZR, BLK)
        F.zf[0:half] = total
        F.zs[0:half] = total.astype(bf16)
        total = F.zf[half:NZ]
        for d in range(1, NY):
            arrived(F.sx.at[d - 1], F.rtx.at[d - 1])
            total = total + F.sx[d - 1].astype(f32).reshape(half, ZR, BLK)
        F.zf[half:NZ] = total
        F.zs[half:NZ] = total.astype(bf16)
        for d in (4, 3, 5, 2, 6, 1, 7):
            zz = at(z + d, NZ)
            start(F.zs.at[zz], F.rz.at[d - 1], F.rzs.at[d - 1], z=zz)

    def z_sum(F):
        total = F.zf[z]
        for d in (1, 7, 2, 6, 3, 5, 4):
            arrived(F.rz.at[d - 1], F.rzs.at[d - 1])
            total = total + F.rz[d - 1].astype(f32)
        return total

    def exps(i, carry):
        r = pl.ds(pl.multiple_of(i * 32, 32), 32)
        t = jnp.tanh(prob[r, :] * (1.0 / soft_cap))
        e = jnp.exp(soft_cap * t - soft_cap)
        q = 1.0 - t * t
        total = jnp.zeros((32, 128), f32)
        found_e = jnp.zeros((32, 128), f32)
        found_q = jnp.zeros((32, 128), f32)
        for k in range(VROWS // 128):
            s = slice(128 * k, 128 * k + 128)
            hit = hm[r, s].astype(f32) > 0.5
            v = jnp.where(hit, 0.0, e[:, s] * q[:, s])
            prob[r, s] = v
            pm[r, s] = v.astype(bf16)
            total = total + e[:, s]
            found_e = found_e + jnp.where(hit, e[:, s], 0.0)
            found_q = found_q + jnp.where(hit, q[:, s], 0.0)
        sums[r, :] = total
        fe[r, :] = found_e
        fq[r, :] = found_q
        return carry

    for k, step in enumerate((
        ((PLUS, P4), (MINUS, P3), (MINUS, P2), (PLUS, P1)), ((MINUS, P4), (PLUS, P3), (PLUS, R2), (PLUS, L2), (PLUS, ZD)),
        ((MINUS, R1), (MINUS, L1), (MINUS, ZU), (FAR, P2), (FAR, P1)), ((FAR, P4), (FAR, P3)),
    )):
        for s, p in step:
            got(s, p)
        product(T, k)
    for s, p in ((MINUS, R2), (MINUS, L2), (MINUS, ZD), (PLUS, ZU), (PLUS, R1), (PLUS, L1)):
        got(s, p)
    arrived(shard(1, OWN), rd.at[3 * NP])
    from_partner(P1, P2)
    logits(k0, True)
    for i in range(NX):
        of_chip(T, i)
        far_halves(T, i)
    for p in (R2, L2, ZD, R1, L1, ZU):
        got(FAR, p)
    from_partner(P3, R2, R1)
    logits(kp, False)
    from_partner(P4, L2, L1)
    logits(km, False)
    near_x(T)
    for i in range(NX):
        near_y(T, i)
    from_partner(ZD, ZU)
    logits(k2, False)
    lax.fori_loop(0, TOKENS // 32, exps, 0)

    first_part = len(sends)

    def stats():
        for k in range(TOKENS // 128):
            r = slice(128 * k, 128 * k + 128)
            three = [jnp.sum(v[r, :].T, axis=0, keepdims=True) for v in (sums, fe, fq)]
            for j in range(2):
                lanes = slice(ROWS * j, ROWS * j + ROWS)
                stat[pl.ds(group(*RHO[2 * k + j]), 1), :] = jnp.concatenate([v[:, lanes] for v in three] + [none], 1)
        for k, (dy, dc) in enumerate(yc_peers):
            start(stat, b1.at[k], rb.at[k], y=at(y + dy, NY), c=at(c + dc, NC))

    n1 = len(yc_peers)
    n2 = n1 + NX - 1
    product(A, 0)
    stats()
    product(A, 1)
    product(A, 2)
    of_chip(A, 0)
    far_halves(A, 0)
    product(A, 3)
    for i in (1, 2):
        of_chip(A, i)
        far_halves(A, i)
    of_chip(A, 3)
    far_halves(A, 3)
    total = stat[...]
    for k in range(n1):
        arrived(b1.at[k], rb.at[k])
        total = total + b1[k]
    stat2[...] = total
    for d in range(1, NX):
        start(stat2, b2.at[d - 1], rb.at[n1 + d - 1], x=at(x + d, NX))
    near_x(A)
    near_y(A, 0)
    for i in range(1, NX):
        near_y(A, i)
    total = stat2[...]
    for d in range(1, NX):
        arrived(b2.at[d - 1], rb.at[n1 + d - 1])
        total = total + b2[d - 1]
    stat3[...] = total
    for d in (4, 3, 5, 2, 6, 1, 7):
        start(stat3, b3.at[d - 1], rb.at[n2 + d - 1], z=at(z + d, NZ))
    second_part = len(sends)
    stage_two(T)
    drain(first_part)

    total = stat3[...]
    for d in range(1, NZ):
        arrived(b3.at[d - 1], rb.at[n2 + d - 1])
        total = total + b3[d - 1]
    every, e_hit, q_hit = (total[:, ROWS * k : ROWS * k + ROWS] for k in range(3))
    w = wall[:, 0:ROWS]
    factor = w * (1.0 + 2.0 * z_weight * (soft_cap + jnp.log(every))) / every
    rate[...] = jnp.concatenate([factor, (factor * e_hit - w) * q_hit], 1)
    for k in range(TOKENS // 128):
        r = slice(128 * k, 128 * k + 128)
        pair = [rate[pl.ds(group(*RHO[2 * k + j]), 1), :] for j in range(2)]
        frep[r, :] = over_rows([v[:, 0:ROWS] for v in pair])
        hrep[r, :] = over_rows([v[:, ROWS:] for v in pair])

    def scores(i, carry):
        r = pl.ds(pl.multiple_of(i * 32, 32), 32)
        f, h = frep[r, :], hrep[r, :]
        for k in range(VROWS // 128):
            s = slice(128 * k, 128 * k + 128)
            sc[r, s] = f * prob[r, s] + h * hm[r, s].astype(f32)
        return carry

    def table(i):
        tg_out[:, i * BLK : (i + 1) * BLK] = jnp.dot(
            sct[...], hid[:, i * BLK : (i + 1) * BLK], preferred_element_type=f32
        ).astype(bf16)

    lax.fori_loop(0, TOKENS // 32, scores, 0)
    for k in range(VROWS // 128):
        s = slice(128 * k, 128 * k + 128)
        sct[s, :] = sc[:, s].T.astype(bf16)
    table(0)
    stage_two(A)
    to_z(T)
    table(1)
    table(2)
    to_z(A)
    table(3)
    drain(second_part)
    mine = pl.ds(pl.multiple_of(z * ZR, ZR), ZR)
    t_part = z_sum(T)
    a_part = z_sum(A)
    f, h = frep[mine, :], hrep[mine, :]
    for k in range(BLK // 128):
        s = slice(128 * k, 128 * k + 128)
        gz[z, :, s] = (f * a_part[:, s] + h * t_part[:, s]).astype(bf16)
    for d in (4, 3, 5, 2, 6, 1, 7):
        start(gz.at[z], gz.at[z], rzg.at[d - 1], z=at(z + d, NZ))

    def on_to_x(d, zz):
        for dx in (2, 1, 3):
            start(gz.at[zz], gx.at[dx - 1, zz], rxg.at[(dx - 1) * NZ + d], x=at(x + dx, NX))

    on_to_x(0, z)
    for d in (1, 7, 2, 6, 3, 5, 4):
        arrived(gz.at[at(z - d, NZ)], rzg.at[d - 1])
        on_to_x(d, at(z - d, NZ))
    hg_out[:, cols(x)] = gz[...].reshape(ROWS, BLK)
    for dx in range(1, NX):
        for d in range(NZ):
            arrived(gx.at[dx - 1, at(z - d, NZ)], rxg.at[(dx - 1) * NZ + d])
        hg_out[:, cols(at(x - dx, NX))] = gx[dx - 1].reshape(ROWS, BLK)

    drain(len(sends))


def body(hidden, embedding, targets, loss_weight):
    vm = pltpu.VMEM
    dma = pltpu.SemaphoreType.DMA
    inputs = (hidden, embedding, loss_weight.reshape(1, ROWS), targets.reshape(1, ROWS))
    return pl.pallas_call(
        kernel,
        out_shape=(
            jax.ShapeDtypeStruct((ROWS, D), bf16),
            jax.ShapeDtypeStruct((VROWS, D), bf16),
        ),
        in_specs=[pl.BlockSpec(memory_space=pl.ANY)] * 4,
        out_specs=(pl.BlockSpec(memory_space=pltpu.VMEM), pl.BlockSpec(memory_space=pltpu.VMEM)),
        scratch_shapes=[
            vm((1, ROWS), bf16),
            vm((1, ROWS), jnp.int32),
            vm((TOKENS, D), bf16),
            vm((VROWS, D), bf16),
            vm((NC * NY, 2, 128), f32),
            vm((NC * NY, 128), f32),
            vm((TOKENS, 128), f32),
            vm((TOKENS, VROWS), f32),
            vm((TOKENS, 128), f32),
            vm((TOKENS, 128), f32),
            vm((TOKENS, 128), f32),
            vm((NC * NY, 256), f32),
            vm((NC * NY, 256), f32),
            vm((NC * NY, 256), f32),
            vm((NC * NY, 128), f32),
            vm((TOKENS, 128), f32),
            vm((TOKENS, 128), f32),
            vm((NY * NC - 1, NC * NY, 256), f32),
            vm((NX - 1, NC * NY, 256), f32),
            vm((NZ - 1, NC * NY, 256), f32),
            vm((TOKENS, VROWS), bf16),
            vm((TOKENS, VROWS), bf16),
            vm((TOKENS, VROWS), f32),
            vm((VROWS, TOKENS), bf16),
            vm((NX, HALF, BLK), f32),
            vm((NX, HALF, BLK), bf16),
            vm((NX, HALF, BLK), bf16),
            vm((NX, HALF, BLK), bf16),
            vm((NX, HALF, BLK), bf16),
            vm((NX, HALF, BLK), bf16),
            vm((NZ, ZR, BLK), bf16),
            vm((NX - 1, NZ, ZR, BLK), bf16),
            dma((NX + 3,)),
            dma((230,)),
            dma((30,)),
            dma((31,)),
            dma((NY * NC - 1,)),
            dma((NY * NC + NX + NZ - 3,)),
            dma((NZ - 1,)),
            dma(((NX - 1) * NZ,)),
        ]
        + 2
        * [
            vm((2, NX, SUB // 2, BLK), bf16),
            vm((2, NX, SUB // 2, BLK), bf16),
            vm((2, NX, SUB, BLK), bf16),
            vm((2, NX, SUB, BLK), bf16),
            vm((2, NY, SUB // 2, BLK), bf16),
            vm((2, NY, SUB // 2, BLK), bf16),
            vm((2, NY, SUB, BLK), bf16),
            vm((2, NY, SUB, BLK), bf16),
            vm((NX - 1, SUB, BLK), bf16),
            vm((NY - 1, SUB, BLK), bf16),
            vm((NX - 1, SUB, BLK), bf16),
            vm((NY - 1, SUB, BLK), bf16),
            vm((NZ, ZR, BLK), f32),
            vm((NZ, ZR, BLK), bf16),
            vm((NZ - 1, ZR, BLK), bf16),
            dma((NX,)),
            dma((2 * NX,)),
            dma((2 * NX,)),
            dma((2,)),
            dma((2,)),
            dma((NX - 1,)),
            dma((NY - 1,)),
            dma((NZ - 1,)),
        ],
        compiler_params=pltpu.CompilerParams(collective_id=0, has_side_effects=True, vmem_limit_bytes=44 * 1024 * 1024),
        name="head_backward",
    )(*(pltpu.with_memory_space_constraint(a, pltpu.HBM) for a in inputs))


def solution(mesh):
    finer = Mesh(mesh.devices.reshape(NY, NC, NX, NZ), ("y", "c", "x", "z"))
    dp = ("y", "c")
    both = ("y", "c", "x", "z")
    return jax.shard_map(
        body,
        mesh=finer,
        in_specs=(P(dp, None), P(both, None), P(dp), P(dp)),
        out_specs=(P(dp, None), P(both, None)),
        check_vma=False,
    )
```

```python
import functools

import jax
import jax.numpy as jnp
from jax import lax
from jax.experimental import pallas as pl
from jax.experimental.pallas import tpu as pltpu
from jax.sharding import Mesh
from jax.sharding import PartitionSpec as P

MESH = pl.DeviceIdType.MESH
f32, bf16 = jnp.float32, jnp.bfloat16

NY, NC, NX, NZ = 4, 2, 4, 8
D, VROWS, ROWS = 3584, 768, 64
TOKENS = ROWS * NY * NC
HALF = ROWS * NY
BLK = D // NX
SUB = ROWS // 2
ZR = ROWS // NZ
ORDER = (2, 1, 3, 0)

soft_cap = 30.0
z_weight = 0.002


class Field:
    pass


BUFS = ("fy", "fyr", "ny", "nyr", "fx", "fxr", "nx", "nxr", "ys", "xs2", "sy", "sx", "zf", "zs", "rz")
SEMS = ("rd2", "rfy", "rny", "rfx", "rnx", "rty", "rtx", "rzs")


def kernel(
    hid_in, emb_in, w_in, t_in, hg_out, tg_out,
    w_own, t_own, hid, emb, wtb, wall, trep, prob, sums, fe, fq, stat, stat2, stat3, rate, frep, hrep, b1, b2, b3,
    pm, hm, sc, sct, own, town, asend, arecv, tsend, trecv, gz, gx,
    local_sem, send_sem, ra, rd, rw, rb, rzg, rxg, *fields,
):
    A, T = Field(), Field()
    n = len(BUFS) + len(SEMS)
    for field, refs in ((A, fields[:n]), (T, fields[n:])):
        for name, ref in zip(BUFS + SEMS, refs):
            setattr(field, name, ref)
    A.own, A.send, A.recv, A.m = own, asend, arecv, pm
    T.own, T.send, T.recv, T.m = town, tsend, trecv, hm
    y, c, x, z = (lax.axis_index(a) for a in ("y", "c", "x", "z"))
    rem = lax.rem

    def at(i, n):
        return rem(i + n, n)

    up, down, far = at(y + 1, NY), at(y - 1, NY), at(y + 2, NY)
    right, left = at(x + 1, NX), at(x - 1, NX)
    above, below = at(z + 1, NZ), at(z - 1, NZ)
    OWN, PLUS, MINUS, FAR = range(4)
    where = {OWN: y, PLUS: up, MINUS: down, FAR: far}
    RHO = ((0, OWN), (0, PLUS), (0, MINUS), (0, FAR), (1, FAR), (1, OWN), (1, PLUS), (1, MINUS))
    row_of = {key: ROWS * k for k, key in enumerate(RHO)}
    me = c * NY + y

    def group(e, s):
        return (1 - c if e else c) * NY + where[s]

    sends = []

    def start(src, dst, rsem, **dev):
        copy = pltpu.make_async_remote_copy(
            src_ref=src, dst_ref=dst, send_sem=send_sem.at[len(sends)], recv_sem=rsem, device_id=dev, device_id_type=MESH
        )
        copy.start()
        sends.append(copy)

    drained = []

    def drain(until):
        for copy in sends[len(drained) : until]:
            copy.wait_send()
            drained.append(copy)

    def arrived(dst, rsem):
        pltpu.make_async_remote_copy(
            src_ref=dst, dst_ref=dst, send_sem=send_sem.at[0], recv_sem=rsem, device_id={"c": 1 - c}, device_id_type=MESH
        ).wait_recv()

    def cols(q):
        return pl.ds(pl.multiple_of(q * BLK, 128), BLK)

    def shard(e, s):
        return hid.at[row_of[e, s] : row_of[e, s] + ROWS]

    def piece(e, s, q, lo, hi):
        return hid.at[row_of[e, s] : row_of[e, s] + ROWS, pl.ds(pl.multiple_of(q * BLK + lo, 128), hi - lo)]

    load_own = [
        pltpu.make_async_copy(hid_in, shard(0, OWN), local_sem.at[NX]),
        pltpu.make_async_copy(w_in, w_own, local_sem.at[NX + 1]),
        pltpu.make_async_copy(t_in, t_own, local_sem.at[NX + 2]),
    ]
    load_emb = []
    for k in range(NX):
        part = pl.ds(k * (VROWS // NX), VROWS // NX)
        load_emb.append(pltpu.make_async_copy(emb_in.at[part], emb.at[part], local_sem.at[k]))
    for load in load_own + load_emb:
        load.start()

    barrier = pltpu.get_barrier_semaphore()
    yc_peers = [(dy, dc) for dy in range(NY) for dc in range(NC) if (dy, dc) != (0, 0)]
    for dy, dc in yc_peers:
        pl.semaphore_signal(barrier, inc=1, device_id={"y": at(y + dy, NY), "c": at(c + dc, NC)}, device_id_type=MESH)
    for d in range(1, NX):
        pl.semaphore_signal(barrier, inc=1, device_id={"x": at(x + d, NX)}, device_id_type=MESH)
    for d in range(1, NZ):
        pl.semaphore_signal(barrier, inc=1, device_id={"z": at(z + d, NZ)}, device_id_type=MESH)

    for load in load_own:
        load.wait()
    none = jnp.zeros((1, ROWS), f32)
    wtb[me] = jnp.concatenate(
        [jnp.concatenate([v, none], 1) for v in (w_own[...].astype(f32), t_own[...].astype(f32))], 0
    )

    pl.semaphore_wait(barrier, len(yc_peers) + NX - 1 + NZ - 1)

    k0 = rem(x + 2 * z, NX)
    kp, km, k2 = rem(k0 + 1, NX), rem(k0 + 3, NX), rem(k0 + 2, NX)
    P1, P2, P3, P4, R1, R2, L1, L2, ZU, ZD = range(10)
    parts = (
        (k0, 0, 512), (k0, 512, BLK), (kp, 0, 256), (km, 0, 256),
        (kp, 256, 512), (kp, 512, BLK), (km, 256, 512), (km, 512, BLK),
        (k2, 0, 512), (k2, 512, BLK),
    )
    NP = len(parts)

    def slot(s, p):
        return (s - 1) * NP + p

    def to_up(s, p):
        start(piece(0, s, *parts[p]), piece(0, MINUS if s == OWN else FAR, *parts[p]), ra.at[slot(MINUS if s == OWN else FAR, p)], y=up)

    def to_down(s, p):
        start(piece(0, s, *parts[p]), piece(0, PLUS if s == OWN else FAR, *parts[p]), ra.at[slot(PLUS if s == OWN else FAR, p)], y=down)

    for k, (dy, dc) in enumerate(yc_peers):
        start(wtb.at[me], wtb.at[me], rw.at[k], y=at(y + dy, NY), c=at(c + dc, NC))
    for p, q in ((P1, P2), (P3, P4), (P2, P1), (P4, P3)):
        to_up(OWN, p)
        to_down(OWN, q)
    start(shard(0, OWN), shard(1, OWN), rd.at[3 * NP], c=1 - c)

    def got(s, p):
        part = piece(0, s, *parts[p])
        arrived(part, ra.at[slot(s, p)])
        if s == MINUS and p in (P1, P3):
            to_up(s, p)
        if s == PLUS and p in (P2, P4):
            to_down(s, p)
        if p in (P1, P2):
            sub = piece(0, s, k0, 256, 512) if p == P1 else part
            start(sub, sub, ra.at[slot(s, R1 if p == P1 else R2)], x=left)
            start(sub, sub, ra.at[slot(s, L1 if p == P1 else L2)], x=right)
            if p == P1:
                start(part, part, ra.at[slot(s, ZU)], z=below)
            else:
                start(part, part, ra.at[slot(s, ZD)], z=above)
        start(part, piece(1, s, *parts[p]), rd.at[slot(s, p)], c=1 - c)

    def from_partner(*ps):
        for p in ps:
            for s in (PLUS, MINUS, FAR):
                arrived(piece(1, s, *parts[p]), rd.at[slot(s, p)])

    def logits(q, first_one):
        out = lax.dot_general(
            hid[:, cols(q)], emb[:, cols(q)], (((1,), (1,)), ((), ())), preferred_element_type=f32
        )
        prob[...] = out if first_one else prob[...] + out

    def over_rows(pair):
        return jnp.broadcast_to(jnp.concatenate(pair, 1), (128, 128)).T

    for s, p in ((PLUS, P2), (MINUS, P1)):
        got(s, p)

    for load in load_emb:
        load.wait()
    for k, (dy, dc) in enumerate(yc_peers):
        arrived(wtb.at[at(c - dc, NC) * NY + at(y - dy, NY)], rw.at[k])
    for k in range(TOKENS // 128):
        trep[128 * k : 128 * k + 128, :] = over_rows([wtb[group(*RHO[2 * k + j]), 1:2, 0:ROWS] for j in range(2)])
    for g in range(NC * NY):
        wall[g : g + 1, :] = wtb[g, 0:1, :]

    base = ((((y * NC + c) * NX + x) * NZ + z) * VROWS).astype(f32)

    def onehots(i, carry):
        r = pl.ds(pl.multiple_of(i * 32, 32), 32)
        want = trep[r, :] - base
        lane = lax.broadcasted_iota(jnp.int32, (32, 128), 1).astype(f32)
        for k in range(VROWS // 128):
            s = slice(128 * k, 128 * k + 128)
            hm[r, s] = jnp.where(want == lane + float(128 * k), 1.0, 0.0).astype(bf16)
        return carry

    lax.fori_loop(0, TOKENS // 32, onehots, 0)

    blocks = [at(x + d, NX) for d in ORDER]

    def product(F, i):
        v = jnp.dot(F.m[...], emb[:, cols(blocks[i])], preferred_element_type=f32)
        F.send[i, 0:192] = v[HALF + 64 :].astype(bf16)
        F.send[i, 192:256] = v[HALF : HALF + 64].astype(bf16)
        start(F.send.at[i], F.recv.at[i], F.rd2.at[i], c=1 - c)
        F.own[i] = v[:HALF].astype(F.own.dtype)

    def of_chip(F, i):
        arrived(F.recv.at[i], F.rd2.at[i])
        F.own[i] = F.own[i] + F.recv[i].astype(F.own.dtype)

    def far_halves(F, i):
        F.fy[0, i] = F.own[i, 192:208, :].astype(bf16)
        F.fy[1, i] = F.own[i, 208:224, :].astype(bf16)
        start(F.fy.at[0, i], F.fyr.at[0, i], F.rfy.at[i], y=up)
        start(F.fy.at[1, i], F.fyr.at[1, i], F.rfy.at[NX + i], y=down)
        if ORDER[i] == 2:
            for s in range(NY):
                F.fx[0, s] = F.own[i, 64 * s + 32 : 64 * s + 48, :].astype(bf16)
                F.fx[1, s] = F.own[i, 64 * s + 48 : 64 * s + 64, :].astype(bf16)
            start(F.fx.at[0], F.fxr.at[0], F.rfx.at[0], x=right)
            start(F.fx.at[1], F.fxr.at[1], F.rfx.at[1], x=left)

    def with_far(F, i, lo, side, more):
        a1 = F.own[i, lo : lo + 16, :].astype(f32)
        a2 = F.own[i, lo + 16 : lo + 32, :].astype(f32)
        more = more.astype(f32)
        return (a1 + more if side == 0 else a1).astype(bf16), (a2 + more if side == 1 else a2).astype(bf16)

    def near_x(F):
        for side, (b, dev) in enumerate(((1, right), (2, left))):
            arrived(F.fxr.at[side], F.rfx.at[side])
            for s in range(NY):
                F.nx[side, s, 0:16], F.nx[side, s, 16:32] = with_far(F, b, 64 * s + 32, side, F.fxr[side, s])
            start(F.nx.at[side], F.nxr.at[side], F.rnx.at[side], x=dev)

    def near_y(F, i):
        for side, (lo, dev) in enumerate(((64, up), (128, down))):
            arrived(F.fyr.at[side, i], F.rfy.at[side * NX + i])
            F.ny[side, i, 0:16], F.ny[side, i, 16:32] = with_far(F, i, lo, side, F.fyr[side, i])
            start(F.ny.at[side, i], F.nyr.at[side, i], F.rny.at[side * NX + i], y=dev)

    half = NZ // 2

    def stage_two(F):
        for i, d in enumerate(ORDER):
            total = F.own[i, 0:32, :].astype(f32)
            for side in range(2):
                arrived(F.nyr.at[side, i], F.rny.at[side * NX + i])
                total = total + F.nyr[side, i].astype(f32)
            if d:
                F.ys[d - 1] = total.astype(bf16)
                start(F.ys.at[d - 1], F.sy.at[d - 1], F.rty.at[d - 1], x=blocks[i])
            else:
                F.zf[0:half] = total.reshape(half, ZR, BLK)
        for side in range(2):
            arrived(F.nxr.at[side], F.rnx.at[side])
        for s, dy in ((FAR, 2), (PLUS, 1), (MINUS, 3), (OWN, 0)):
            total = F.own[NX - 1, 64 * s_row[s] + 32 : 64 * s_row[s] + 64, :].astype(f32)
            total = total + F.nxr[0, s_row[s]].astype(f32) + F.nxr[1, s_row[s]].astype(f32)
            if dy:
                F.xs2[dy - 1] = total.astype(bf16)
                start(F.xs2.at[dy - 1], F.sx.at[dy - 1], F.rtx.at[dy - 1], y=where[s])
            else:
                F.zf[half:NZ] = total.reshape(half, ZR, BLK)

    s_row = {s: row_of[0, s] // ROWS for s in range(4)}

    def to_z(F):
        total = F.zf[0:half]
        for d in range(1, NX):
            arrived(F.sy.at[d - 1], F.rty.at[d - 1])
            total = total + F.sy[d - 1].astype(f32).reshape(half, ZR, BLK)
        F.zf[0:half] = total
        F.zs[0:half] = total.astype(bf16)
        total = F.zf[half:NZ]
        for d in range(1, NY):
            arrived(F.sx.at[d - 1], F.rtx.at[d - 1])
            total = total + F.sx[d - 1].astype(f32).reshape(half, ZR, BLK)
        F.zf[half:NZ] = total
        F.zs[half:NZ] = total.astype(bf16)
        for d in (4, 3, 5, 2, 6, 1, 7):
            zz = at(z + d, NZ)
            start(F.zs.at[zz], F.rz.at[d - 1], F.rzs.at[d - 1], z=zz)

    def z_sum(F):
        total = F.zf[z]
        for d in (1, 7, 2, 6, 3, 5, 4):
            arrived(F.rz.at[d - 1], F.rzs.at[d - 1])
            total = total + F.rz[d - 1].astype(f32)
        return total

    def exps(i, carry):
        r = pl.ds(pl.multiple_of(i * 32, 32), 32)
        t = jnp.tanh(prob[r, :] * (1.0 / soft_cap))
        e = jnp.exp(soft_cap * t - soft_cap)
        q = 1.0 - t * t
        total = jnp.zeros((32, 128), f32)
        found_e = jnp.zeros((32, 128), f32)
        found_q = jnp.zeros((32, 128), f32)
        for k in range(VROWS // 128):
            s = slice(128 * k, 128 * k + 128)
            hit = hm[r, s].astype(f32) > 0.5
            v = jnp.where(hit, 0.0, e[:, s] * q[:, s])
            prob[r, s] = v
            pm[r, s] = v.astype(bf16)
            total = total + e[:, s]
            found_e = found_e + jnp.where(hit, e[:, s], 0.0)
            found_q = found_q + jnp.where(hit, q[:, s], 0.0)
        sums[r, :] = total
        fe[r, :] = found_e
        fq[r, :] = found_q
        return carry

    for k, step in enumerate((
        ((PLUS, P4), (MINUS, P3), (MINUS, P2), (PLUS, P1)), ((MINUS, P4), (PLUS, P3), (PLUS, R2), (PLUS, L2), (PLUS, ZD)),
        ((MINUS, R1), (MINUS, L1), (MINUS, ZU), (FAR, P2), (FAR, P1)), ((FAR, P4), (FAR, P3)),
    )):
        for s, p in step:
            got(s, p)
        product(T, k)
    for s, p in ((MINUS, R2), (MINUS, L2), (MINUS, ZD), (PLUS, ZU), (PLUS, R1), (PLUS, L1)):
        got(s, p)
    arrived(shard(1, OWN), rd.at[3 * NP])
    from_partner(P1, P2)
    logits(k0, True)
    for i in range(NX):
        of_chip(T, i)
        far_halves(T, i)
    for p in (R2, L2, ZD, R1, L1, ZU):
        got(FAR, p)
    from_partner(P3, R2, R1)
    logits(kp, False)
    from_partner(P4, L2, L1)
    logits(km, False)
    near_x(T)
    for i in range(NX):
        near_y(T, i)
    from_partner(ZD, ZU)
    logits(k2, False)
    lax.fori_loop(0, TOKENS // 32, exps, 0)

    first_part = len(sends)

    def stats():
        for k in range(TOKENS // 128):
            r = slice(128 * k, 128 * k + 128)
            three = [jnp.sum(v[r, :].T, axis=0, keepdims=True) for v in (sums, fe, fq)]
            for j in range(2):
                lanes = slice(ROWS * j, ROWS * j + ROWS)
                stat[pl.ds(group(*RHO[2 * k + j]), 1), :] = jnp.concatenate([v[:, lanes] for v in three] + [none], 1)
        for k, (dy, dc) in enumerate(yc_peers):
            start(stat, b1.at[k], rb.at[k], y=at(y + dy, NY), c=at(c + dc, NC))

    n1 = len(yc_peers)
    n2 = n1 + NX - 1
    product(A, 0)
    stats()
    product(A, 1)
    product(A, 2)
    of_chip(A, 0)
    far_halves(A, 0)
    product(A, 3)
    for i in (1, 2):
        of_chip(A, i)
        far_halves(A, i)
    of_chip(A, 3)
    far_halves(A, 3)
    total = stat[...]
    for k in range(n1):
        arrived(b1.at[k], rb.at[k])
        total = total + b1[k]
    stat2[...] = total
    for d in range(1, NX):
        start(stat2, b2.at[d - 1], rb.at[n1 + d - 1], x=at(x + d, NX))
    near_x(A)
    near_y(A, 0)
    for i in range(1, NX):
        near_y(A, i)
    total = stat2[...]
    for d in range(1, NX):
        arrived(b2.at[d - 1], rb.at[n1 + d - 1])
        total = total + b2[d - 1]
    stat3[...] = total
    for d in (4, 3, 5, 2, 6, 1, 7):
        start(stat3, b3.at[d - 1], rb.at[n2 + d - 1], z=at(z + d, NZ))
    second_part = len(sends)
    stage_two(T)
    drain(first_part)

    total = stat3[...]
    for d in range(1, NZ):
        arrived(b3.at[d - 1], rb.at[n2 + d - 1])
        total = total + b3[d - 1]
    every, e_hit, q_hit = (total[:, ROWS * k : ROWS * k + ROWS] for k in range(3))
    w = wall[:, 0:ROWS]
    factor = w * (1.0 + 2.0 * z_weight * (soft_cap + jnp.log(every))) / every
    rate[...] = jnp.concatenate([factor, (factor * e_hit - w) * q_hit], 1)
    for k in range(TOKENS // 128):
        r = slice(128 * k, 128 * k + 128)
        pair = [rate[pl.ds(group(*RHO[2 * k + j]), 1), :] for j in range(2)]
        frep[r, :] = over_rows([v[:, 0:ROWS] for v in pair])
        hrep[r, :] = over_rows([v[:, ROWS:] for v in pair])

    def scores(i, carry):
        r = pl.ds(pl.multiple_of(i * 32, 32), 32)
        f, h = frep[r, :], hrep[r, :]
        for k in range(VROWS // 128):
            s = slice(128 * k, 128 * k + 128)
            sc[r, s] = f * prob[r, s] + h * hm[r, s].astype(f32)
        return carry

    def table(i):
        tg_out[:, i * BLK : (i + 1) * BLK] = jnp.dot(
            sct[...], hid[:, i * BLK : (i + 1) * BLK], preferred_element_type=f32
        ).astype(bf16)

    lax.fori_loop(0, TOKENS // 32, scores, 0)
    for k in range(VROWS // 128):
        s = slice(128 * k, 128 * k + 128)
        sct[s, :] = sc[:, s].T.astype(bf16)
    table(0)
    stage_two(A)
    to_z(T)
    table(1)
    table(2)
    to_z(A)
    table(3)
    drain(second_part)
    mine = pl.ds(pl.multiple_of(z * ZR, ZR), ZR)
    t_part = z_sum(T)
    a_part = z_sum(A)
    f, h = frep[mine, :], hrep[mine, :]
    for k in range(BLK // 128):
        s = slice(128 * k, 128 * k + 128)
        gz[z, :, s] = (f * a_part[:, s] + h * t_part[:, s]).astype(bf16)
    for d in (1, 7, 2, 6, 3, 5, 4):
        start(gz.at[z], gz.at[z], rzg.at[d - 1], z=at(z + d, NZ))

    def on_to_x(d, zz):
        for dx in (2, 1, 3):
            start(gz.at[zz], gx.at[dx - 1, zz], rxg.at[(dx - 1) * NZ + d], x=at(x + dx, NX))

    on_to_x(0, z)
    for d in (1, 7, 2, 6, 3, 5, 4):
        arrived(gz.at[at(z - d, NZ)], rzg.at[d - 1])
        on_to_x(d, at(z - d, NZ))
    hg_out[:, cols(x)] = gz[...].reshape(ROWS, BLK)
    for dx in range(1, NX):
        for d in range(NZ):
            arrived(gx.at[dx - 1, at(z - d, NZ)], rxg.at[(dx - 1) * NZ + d])
        hg_out[:, cols(at(x - dx, NX))] = gx[dx - 1].reshape(ROWS, BLK)

    drain(len(sends))


def body(hidden, embedding, targets, loss_weight):
    vm = pltpu.VMEM
    dma = pltpu.SemaphoreType.DMA
    inputs = (hidden, embedding, loss_weight.reshape(1, ROWS), targets.reshape(1, ROWS))
    return pl.pallas_call(
        kernel,
        out_shape=(
            jax.ShapeDtypeStruct((ROWS, D), bf16),
            jax.ShapeDtypeStruct((VROWS, D), bf16),
        ),
        in_specs=[pl.BlockSpec(memory_space=pl.ANY)] * 4,
        out_specs=(pl.BlockSpec(memory_space=pltpu.VMEM), pl.BlockSpec(memory_space=pltpu.VMEM)),
        scratch_shapes=[
            vm((1, ROWS), bf16),
            vm((1, ROWS), jnp.int32),
            vm((TOKENS, D), bf16),
            vm((VROWS, D), bf16),
            vm((NC * NY, 2, 128), f32),
            vm((NC * NY, 128), f32),
            vm((TOKENS, 128), f32),
            vm((TOKENS, VROWS), f32),
            vm((TOKENS, 128), f32),
            vm((TOKENS, 128), f32),
            vm((TOKENS, 128), f32),
            vm((NC * NY, 256), f32),
            vm((NC * NY, 256), f32),
            vm((NC * NY, 256), f32),
            vm((NC * NY, 128), f32),
            vm((TOKENS, 128), f32),
            vm((TOKENS, 128), f32),
            vm((NY * NC - 1, NC * NY, 256), f32),
            vm((NX - 1, NC * NY, 256), f32),
            vm((NZ - 1, NC * NY, 256), f32),
            vm((TOKENS, VROWS), bf16),
            vm((TOKENS, VROWS), bf16),
            vm((TOKENS, VROWS), f32),
            vm((VROWS, TOKENS), bf16),
            vm((NX, HALF, BLK), f32),
            vm((NX, HALF, BLK), bf16),
            vm((NX, HALF, BLK), bf16),
            vm((NX, HALF, BLK), bf16),
            vm((NX, HALF, BLK), bf16),
            vm((NX, HALF, BLK), bf16),
            vm((NZ, ZR, BLK), bf16),
            vm((NX - 1, NZ, ZR, BLK), bf16),
            dma((NX + 3,)),
            dma((230,)),
            dma((30,)),
            dma((31,)),
            dma((NY * NC - 1,)),
            dma((NY * NC + NX + NZ - 3,)),
            dma((NZ - 1,)),
            dma(((NX - 1) * NZ,)),
        ]
        + 2
        * [
            vm((2, NX, SUB // 2, BLK), bf16),
            vm((2, NX, SUB // 2, BLK), bf16),
            vm((2, NX, SUB, BLK), bf16),
            vm((2, NX, SUB, BLK), bf16),
            vm((2, NY, SUB // 2, BLK), bf16),
            vm((2, NY, SUB // 2, BLK), bf16),
            vm((2, NY, SUB, BLK), bf16),
            vm((2, NY, SUB, BLK), bf16),
            vm((NX - 1, SUB, BLK), bf16),
            vm((NY - 1, SUB, BLK), bf16),
            vm((NX - 1, SUB, BLK), bf16),
            vm((NY - 1, SUB, BLK), bf16),
            vm((NZ, ZR, BLK), f32),
            vm((NZ, ZR, BLK), bf16),
            vm((NZ - 1, ZR, BLK), bf16),
            dma((NX,)),
            dma((2 * NX,)),
            dma((2 * NX,)),
            dma((2,)),
            dma((2,)),
            dma((NX - 1,)),
            dma((NY - 1,)),
            dma((NZ - 1,)),
        ],
        compiler_params=pltpu.CompilerParams(collective_id=0, has_side_effects=True, vmem_limit_bytes=44 * 1024 * 1024),
        name="head_backward",
    )(*(pltpu.with_memory_space_constraint(a, pltpu.HBM) for a in inputs))


def solution(mesh):
    finer = Mesh(mesh.devices.reshape(NY, NC, NX, NZ), ("y", "c", "x", "z"))
    dp = ("y", "c")
    both = ("y", "c", "x", "z")
    return jax.shard_map(
        body,
        mesh=finer,
        in_specs=(P(dp, None), P(both, None), P(dp), P(dp)),
        out_specs=(P(dp, None), P(both, None)),
        check_vma=False,
    )
```
